32 devices in a mesh: dp: 1 (over z), tp: 4 (over y), cp: 8 (over x, core).
Axes of the slice: x: 4, y: 4, z: 1, core: 2. Of those that a mesh axis runs over, the one named last changes fastest.
The devices are a block of a 4x4x8 slice.
Arguments:
- hidden_in: bfloat16 [512, 3072], P(('dp', 'cp', 'tp'))
- positions: int32 [512], P(('dp', 'cp', 'tp'))
- cache_len: int32 [1], P('dp')
- cache_k: bfloat16 [32768, 1024], P(('dp', 'cp', 'tp'))
- cache_v: bfloat16 [32768, 1024], P(('dp', 'cp', 'tp'))
- norm1_gain: bfloat16 [3072], replicated
- w_query: bfloat16 [3072, 3072], P(None, 'tp')
- w_key: bfloat16 [3072, 1024], P(None, 'tp')
- w_value: bfloat16 [3072, 1024], P(None, 'tp')
- w_out: bfloat16 [3072, 3072], P('tp')
- norm2_gain: bfloat16 [3072], replicated
- w_gate: bfloat16 [3072, 8192], P(None, 'tp')
- w_up: bfloat16 [3072, 8192], P(None, 'tp')
- w_down: bfloat16 [8192, 3072], P('tp')
Outputs:
- output: bfloat16 [512, 3072], P(('dp', 'cp', 'tp'))
All inputs are finite; a program needn't handle non-finite values.
Results may differ from the reference program's by a relative error of at most 0.0110867.
Values are sent between devices in bfloat16 or wider.
A program may use at most 768 MiB of HBM per device.

```python
import math
import jax
import jax.numpy as jnp
from jax import lax

TOKENS = 512
PREFIX = 32768
D_MODEL = 3072
Q_HEADS = 24
KV_HEADS = 8
HEAD_DIM = 128
FFN_DIM = 8192
SHARD_COUNT = 32
SHARD_ROWS = 16
QUERY_BLOCK = 16
ROPE_BASE = 500000.0
NORM_EPS = 1e-5


def normal_draw(rand_key, out_shape, spread):
    return (jax.random.normal(rand_key, out_shape, jnp.float32) * spread).astype(jnp.bfloat16)


def setup_inputs(seed: int = 0, part: int = 0) -> dict:
    base_key = jax.random.key(seed)
    part_keys = jax.random.split(jax.random.fold_in(base_key, part), 4)
    shared_keys = jax.random.split(jax.random.key(seed + 1), 9)
    cache_len = jax.random.randint(part_keys[0], (1,), PREFIX // 16, PREFIX + 1, dtype=jnp.int32)
    row_ids = jnp.arange(TOKENS, dtype=jnp.int32)
    half_rows = SHARD_ROWS // 2
    shard_ids = row_ids // SHARD_ROWS
    within = row_ids % SHARD_ROWS
    segment = jnp.where(within < half_rows, shard_ids, 2 * SHARD_COUNT - 1 - shard_ids)
    positions = cache_len[0] + segment * half_rows + within % half_rows
    qk_std = math.log((PREFIX + TOKENS) / 4.0) ** 0.25
    width_std = D_MODEL ** -0.5
    kv_width = KV_HEADS * HEAD_DIM
    return {
        'hidden_in': normal_draw(part_keys[1], (TOKENS, D_MODEL), 1.0),
        'positions': positions,
        'cache_len': cache_len,
        'cache_k': normal_draw(part_keys[2], (PREFIX, kv_width), qk_std),
        'cache_v': normal_draw(part_keys[3], (PREFIX, kv_width), 1.0),
        'norm1_gain': (1.0 + 0.3 * jax.random.normal(shared_keys[0], (D_MODEL,), jnp.float32)).astype(jnp.bfloat16),
        'w_query': normal_draw(shared_keys[1], (D_MODEL, Q_HEADS * HEAD_DIM), qk_std * width_std),
        'w_key': normal_draw(shared_keys[2], (D_MODEL, kv_width), qk_std * width_std),
        'w_value': normal_draw(shared_keys[3], (D_MODEL, kv_width), width_std),
        'w_out': normal_draw(shared_keys[4], (Q_HEADS * HEAD_DIM, D_MODEL), 2.0 * (Q_HEADS * HEAD_DIM) ** -0.5),
        'norm2_gain': (1.0 + 0.3 * jax.random.normal(shared_keys[5], (D_MODEL,), jnp.float32)).astype(jnp.bfloat16),
        'w_gate': normal_draw(shared_keys[6], (D_MODEL, FFN_DIM), width_std),
        'w_up': normal_draw(shared_keys[7], (D_MODEL, FFN_DIM), width_std),
        'w_down': normal_draw(shared_keys[8], (FFN_DIM, D_MODEL), FFN_DIM ** -0.5),
    }


def rms_norm(hidden, norm_gain):
    values = hidden.astype(jnp.float32)
    inv_rms = lax.rsqrt(jnp.mean(values * values, axis=-1, keepdims=True) + NORM_EPS)
    return (values * inv_rms * norm_gain.astype(jnp.float32)).astype(jnp.bfloat16)


def rotary(projected, positions):
    half_dim = HEAD_DIM // 2
    inv_freq = 1.0 / (ROPE_BASE ** (jnp.arange(half_dim, dtype=jnp.float32) * (2.0 / HEAD_DIM)))
    angles = positions.astype(jnp.float32)[:, None] * inv_freq[None, :]
    expand = (angles.shape[0],) + (1,) * (projected.ndim - 2) + (half_dim,)
    cos_table = jnp.cos(angles).reshape(expand)
    sin_table = jnp.sin(angles).reshape(expand)
    first_half = projected[..., :half_dim]
    second_half = projected[..., half_dim:]
    rotated = jnp.concatenate([first_half * cos_table - second_half * sin_table, second_half * cos_table + first_half * sin_table], axis=-1)
    return rotated.astype(jnp.bfloat16)


def reference(hidden_in, positions, cache_len, cache_k, cache_v, norm1_gain, w_query, w_key, w_value, w_out, norm2_gain, w_gate, w_up, w_down):
    groups = Q_HEADS // KV_HEADS
    block_count = TOKENS // QUERY_BLOCK
    score_scale = 1.0 / math.sqrt(HEAD_DIM)
    normed = rms_norm(hidden_in, norm1_gain)
    queries = rotary(jnp.dot(normed, w_query, preferred_element_type=jnp.float32).reshape(TOKENS, KV_HEADS, groups, HEAD_DIM), positions)
    new_keys = rotary(jnp.dot(normed, w_key, preferred_element_type=jnp.float32).reshape(TOKENS, KV_HEADS, HEAD_DIM), positions)
    new_values = jnp.dot(normed, w_value, preferred_element_type=jnp.float32).astype(jnp.bfloat16).reshape(TOKENS, KV_HEADS, HEAD_DIM)
    head_keys = jnp.moveaxis(new_keys, 1, 0)
    head_values = jnp.moveaxis(new_values, 1, 0)
    cached_keys = jnp.moveaxis(cache_k.reshape(PREFIX, KV_HEADS, HEAD_DIM), 1, 0)
    cached_values = jnp.moveaxis(cache_v.reshape(PREFIX, KV_HEADS, HEAD_DIM), 1, 0)
    cache_valid = jnp.arange(PREFIX) < cache_len[0]
    query_blocks = jnp.moveaxis(queries.reshape(block_count, QUERY_BLOCK, KV_HEADS, groups, HEAD_DIM), 2, 1)
    position_blocks = positions.reshape(block_count, QUERY_BLOCK)

    def attend_block(block_item):
        block_queries, block_pos = block_item
        causal = positions[None, None, :] <= block_pos[None, :, None]

        def attend_head(head_item):
            head_queries, cache_key_head, cache_value_head, new_key_head, new_value_head = head_item
            query_wide = head_queries.astype(jnp.float32)
            cache_scores = jnp.einsum('rgd,sd->grs', query_wide, cache_key_head.astype(jnp.float32)) * score_scale
            new_scores = jnp.einsum('rgd,sd->grs', query_wide, new_key_head.astype(jnp.float32)) * score_scale
            cache_scores = jnp.where(cache_valid[None, None, :], cache_scores, -jnp.inf)
            new_scores = jnp.where(causal, new_scores, -jnp.inf)
            row_max = jnp.maximum(jnp.max(cache_scores, axis=-1, keepdims=True), jnp.max(new_scores, axis=-1, keepdims=True))
            cache_probs = jnp.exp(cache_scores - row_max)
            new_probs = jnp.exp(new_scores - row_max)
            normalizer = jnp.sum(cache_probs, axis=-1, keepdims=True) + jnp.sum(new_probs, axis=-1, keepdims=True)
            weighted = jnp.einsum('grs,sd->grd', cache_probs.astype(jnp.bfloat16).astype(jnp.float32), cache_value_head.astype(jnp.float32))
            weighted = weighted + jnp.einsum('grs,sd->grd', new_probs.astype(jnp.bfloat16).astype(jnp.float32), new_value_head.astype(jnp.float32))
            return (weighted / normalizer).astype(jnp.bfloat16)

        return lax.map(attend_head, (block_queries, cached_keys, cached_values, head_keys, head_values))

    attended = lax.map(attend_block, (query_blocks, position_blocks))
    attended = jnp.transpose(attended, (0, 3, 1, 2, 4)).reshape(TOKENS, Q_HEADS * HEAD_DIM)
    residual_mid = (hidden_in.astype(jnp.float32) + jnp.dot(attended, w_out, preferred_element_type=jnp.float32)).astype(jnp.bfloat16)
    normed_mid = rms_norm(residual_mid, norm2_gain)
    gate_proj = jnp.dot(normed_mid, w_gate, preferred_element_type=jnp.float32)
    up_proj = jnp.dot(normed_mid, w_up, preferred_element_type=jnp.float32)
    hidden_mlp = (jax.nn.silu(gate_proj) * up_proj).astype(jnp.bfloat16)
    return (residual_mid.astype(jnp.float32) + jnp.dot(hidden_mlp, w_down, preferred_element_type=jnp.float32)).astype(jnp.bfloat16)
```

```python
import functools
import math

import jax
import jax.numpy as jnp
from jax import lax
from jax.experimental import pallas as pl
from jax.experimental.pallas import tpu as pltpu
from jax.sharding import PartitionSpec as P

HEAD_DIM = 128
ROPE_BASE = 500000.0
NORM_EPS = 1e-5
HIDDEN = -1e38
SCALE2 = math.log2(math.e) / math.sqrt(HEAD_DIM)
MESH = pl.DeviceIdType.MESH
RING = 4
VMEM_LIMIT = 67_043_328


def place():
    c = lax.axis_index('cp')
    return c // 2, lax.axis_index('tp'), lax.rem(c, 2)


def ring(i):
    return lax.rem(i + RING, RING)


def device(x, y, core):
    return {'tp': ring(y), 'cp': 2 * ring(x) + core}


def remote(src, dst, send_sem, recv_sem, target):
    return pltpu.make_async_remote_copy(src_ref=src, dst_ref=dst, send_sem=send_sem, recv_sem=recv_sem, device_id=target, device_id_type=MESH)


def greet(partners):
    barrier = pltpu.get_barrier_semaphore()
    for partner in partners:
        pl.semaphore_signal(barrier, inc=1, device_id=partner, device_id_type=MESH)
    pl.semaphore_wait(barrier, len(partners))


def normalize(values, gain):
    inv_rms = lax.rsqrt(jnp.mean(values * values, axis=-1, keepdims=True) + NORM_EPS)
    return (values * inv_rms * gain.astype(jnp.float32)).astype(jnp.bfloat16)


def dot(a, b):
    return jnp.dot(a, b, preferred_element_type=jnp.float32)


def dot_nt(a, b):
    return lax.dot_general(a, b, (((1,), (1,)), ((), ())), preferred_element_type=jnp.float32)


def project_kernel(x_ref, gain_ref, wq_hbm, wk_hbm, wv_hbm, cos_ref, sin_ref, q_ref, k_ref, v_ref, wq, wk, wv, rows, load_sem, ss, rs):
    x, y, core = place()
    heads = q_ref.shape[0]
    half = rows.shape[-1] // 2
    loads = []
    for i, (src, dst) in enumerate(((wq_hbm, wq), (wk_hbm, wk), (wv_hbm, wv))):
        width = dst.shape[1]
        loads.append(pltpu.make_async_copy(src.at[:, pl.ds(pl.multiple_of(core * width, width), width)], dst, load_sem.at[i]))
        loads[-1].start()
    sibling, up, down = device(x, y, 1 - core), device(x, y + 1, core), device(x, y - 1, core)
    greet((sibling, up, down))
    rows[core, y] = normalize(x_ref[...].astype(jnp.float32), gain_ref[...])
    lo, hi = pl.ds(0, half), pl.ds(half, half)

    def copy(i, block, cols, target):
        ref = rows.at[core, ring(block)] if cols is None else rows.at[core, ring(block), :, cols]
        return remote(ref, ref, ss.at[i], rs.at[i], target)

    to_up, to_down, own = copy(1, y, None, up), copy(2, y, None, down), copy(0, y, None, sibling)
    to_up.start()
    to_down.start()
    own.start()
    pending = [to_up, to_down, own]

    def go(c):
        c.start()
        pending.append(c)
        return c

    def arrived(i, block, cols):
        ref = rows.at[core, ring(block)] if cols is None else rows.at[core, ring(block), :, cols]
        remote(ref, ref, ss.at[i], rs.at[i], up).wait_recv()

    arrived(1, y - 1, None)
    go(copy(4, y - 1, lo, up))
    go(copy(3, y - 1, None, sibling))
    arrived(2, y + 1, None)
    go(copy(6, y + 1, hi, down))
    go(copy(5, y + 1, None, sibling))
    arrived(4, y - 2, lo)
    go(copy(7, y - 2, lo, sibling))
    arrived(6, y + 2, hi)
    go(copy(8, y + 2, hi, sibling))
    other = 1 - core

    def from_sibling(i, block, cols):
        ref = rows.at[other, ring(block)] if cols is None else rows.at[other, ring(block), :, cols]
        remote(ref, ref, ss.at[i], rs.at[i], sibling).wait_recv()

    from_sibling(0, y, None)
    from_sibling(3, y - 1, None)
    from_sibling(5, y + 1, None)
    from_sibling(7, y - 2, lo)
    from_sibling(8, y + 2, hi)
    for load in loads:
        load.wait()
    a = rows[...].reshape(-1, rows.shape[-1])
    cos, sin = cos_ref[...], sin_ref[...]

    def rotate(p):
        return (p * cos + pltpu.roll(p, HEAD_DIM // 2, axis=1) * sin).astype(jnp.bfloat16)

    q = dot(a, wq[...])
    for g in range(heads):
        q_ref[g] = rotate(q[:, g * HEAD_DIM : (g + 1) * HEAD_DIM])
    k_ref[...] = rotate(dot(a, wk[...]))
    v_ref[...] = dot(a, wv[...]).astype(jnp.bfloat16)
    for c in pending:
        c.wait_send()


def project(hidden, gain, w_query, w_key, w_value, cos, sin):
    shard_rows, width = hidden.shape
    kv_local = w_key.shape[1] // HEAD_DIM
    heads = w_query.shape[1] // w_key.shape[1]
    rows = 2 * RING * shard_rows
    assert kv_local == 2
    vmem, hbm = pl.BlockSpec(memory_space=pltpu.VMEM), pl.BlockSpec(memory_space=pl.ANY)
    return pl.pallas_call(
        project_kernel,
        out_shape=[
            jax.ShapeDtypeStruct((heads, rows, HEAD_DIM), jnp.bfloat16),
            jax.ShapeDtypeStruct((rows, HEAD_DIM), jnp.bfloat16),
            jax.ShapeDtypeStruct((rows, HEAD_DIM), jnp.bfloat16),
        ],
        in_specs=[vmem, vmem, hbm, hbm, hbm, vmem, vmem],
        out_specs=[vmem] * 3,
        scratch_shapes=[
            pltpu.VMEM((width, heads * HEAD_DIM), jnp.bfloat16),
            pltpu.VMEM((width, HEAD_DIM), jnp.bfloat16),
            pltpu.VMEM((width, HEAD_DIM), jnp.bfloat16),
            pltpu.VMEM((2, RING, shard_rows, width), jnp.bfloat16),
            pltpu.SemaphoreType.DMA((3,)),
            pltpu.SemaphoreType.DMA((9,)),
            pltpu.SemaphoreType.DMA((9,)),
        ],
        compiler_params=pltpu.CompilerParams(collective_id=0, has_side_effects=True, vmem_limit_bytes=VMEM_LIMIT),
    )(hidden, gain, w_query, w_key, w_value, cos, sin)


def merge(parts):
    top = parts[0][HEAD_DIM : HEAD_DIM + 1]
    for p in parts[1:]:
        top = jnp.maximum(top, p[HEAD_DIM : HEAD_DIM + 1])
    total, norm = 0.0, 0.0
    for p in parts:
        weight = jnp.exp2(p[HEAD_DIM : HEAD_DIM + 1] - top)
        total = total + p[:HEAD_DIM] * weight
        norm = norm + p[HEAD_DIM + 1 : HEAD_DIM + 2] * weight
    return total, top, norm


def put_block(ref, index, total, top, norm):
    ref[(*index, pl.ds(0, HEAD_DIM))] = total
    ref[(*index, pl.ds(HEAD_DIM, 8))] = jnp.concatenate([top, norm, jnp.zeros((6, total.shape[1]), jnp.float32)], axis=0)


def attend_kernel(len_ref, q_in, kn_in, vn_in, ck_hbm, cv_hbm, o_ref, kbuf, vbuf, vt, qbuf, bias, cbias, sbuf, ob, r1, n1, r2, n2, ox, oin, csem, xs, xr, gs, gr, ps, pr, os_, or_):
    x, y, core = place()
    heads = q_in.shape[0]
    slots = ck_hbm.shape[0]
    cached = 2 * slots
    rows = q_in.shape[1]
    half_rows = rows // (4 * RING)
    other = 1 - core
    a1, a2 = x + core * (y - x), y + core * (x - y)
    sibling = device(x, y, other)

    def on1(d):
        return device(x + d * other, y + d * core, core)

    def on2(d):
        return device(x + d * core, y + d * other, core)

    local, cross = [], []
    mine = pl.ds(pl.multiple_of(core * slots, slots), slots)
    for j in range(RING):
        for i, (src, dst) in enumerate(((ck_hbm, kbuf), (cv_hbm, vbuf))):
            cols = pl.ds(pl.multiple_of((2 * j + core) * HEAD_DIM, HEAD_DIM), HEAD_DIM)
            local.append(pltpu.make_async_copy(src.at[:, cols], dst.at[j, mine], csem.at[2 * j + i]))
            local[-1].start()
    greet((sibling, on1(1), on1(-1), on2(1), on2(-1)))

    for g in range(heads):
        qbuf[g, a2, a1] = q_in[g]

    def q1(g, i, block, part, target):
        ref = qbuf.at[g, a2, ring(block)] if part is None else qbuf.at[g, a2, ring(block), part]
        return remote(ref, ref, gs.at[g, i], gr.at[g, i], target)

    def q2(g, i, block, part, target):
        ref = qbuf.at[g, ring(block)] if part is None else qbuf.at[g, ring(block), part]
        return remote(ref, ref, gs.at[g, i], gr.at[g, i], target)

    lo, hi = pl.ds(0, rows // 2), pl.ds(rows // 2, rows // 2)
    two_lo, two_hi = pl.ds(0, 2), pl.ds(2, 2)
    for g in range(heads):
        q1(g, 0, a1, None, on1(1)).start()
        q1(g, 1, a1, None, on1(-1)).start()
    for j in range(RING):
        for i, (src, dst) in enumerate(((ck_hbm, kbuf), (cv_hbm, vbuf))):
            cols = pl.ds(pl.multiple_of((2 * j + other) * HEAD_DIM, HEAD_DIM), HEAD_DIM)
            cross.append(remote(src.at[:, cols], dst.at[j, mine], xs.at[2 * j + i], xr.at[2 * j + i], sibling))
            cross[-1].start()

    def q1_relay(g):
        q1(g, 0, a1 - 1, None, on1(1)).wait_recv()
        q1(g, 2, a1 - 1, lo, on1(1)).start()
        q1(g, 1, a1 + 1, None, on1(1)).wait_recv()
        q1(g, 3, a1 + 1, hi, on1(-1)).start()

    def q1_done(g):
        q1(g, 2, a1 - 2, lo, on1(1)).wait_recv()
        q1(g, 3, a1 + 2, hi, on1(1)).wait_recv()
        q2(g, 4, a2, None, on2(1)).start()
        q2(g, 5, a2, None, on2(-1)).start()

    def q2_relay(g):
        q2(g, 4, a2 - 1, None, on2(1)).wait_recv()
        q2(g, 6, a2 - 1, two_lo, on2(1)).start()
        q2(g, 5, a2 + 1, None, on2(1)).wait_recv()
        q2(g, 7, a2 + 1, two_hi, on2(-1)).start()

    def q2_done(g):
        q2(g, 6, a2 - 2, two_lo, on2(1)).wait_recv()
        q2(g, 7, a2 + 2, two_hi, on2(1)).wait_recv()

    for g in range(heads):
        q1_relay(g)
    for g in range(heads):
        q1_done(g)

    tail = pl.ds(cached, rows)
    for j in range(RING):
        keep = jnp.where(y == j, 1.0, 0.0).astype(jnp.bfloat16)
        kbuf[j, tail] = kn_in[...] * keep
        vbuf[j, tail] = vn_in[...] * keep
    length = len_ref[0]
    for part in range(2):
        base = ((2 * x + part) * RING + y) * slots
        slot = base + lax.broadcasted_iota(jnp.int32, (slots, HEAD_DIM), 0)
        bias[pl.ds(part * slots, slots)] = jnp.where(slot < length, 0.0, HIDDEN)

    def order(i, xg):
        c_part, rest = i // (rows // 2), lax.rem(i, rows // 2)
        t_part, r = rest // (2 * half_rows), lax.rem(rest, 2 * half_rows)
        owner = (2 * xg + c_part) * RING + t_part
        run = jnp.where(r < half_rows, owner, 4 * RING * RING - 1 - owner)
        return run * half_rows + lax.rem(r, half_rows)

    key_order = order(lax.broadcasted_iota(jnp.int32, (rows, rows), 0), x)
    for xg in range(RING):
        query_order = order(lax.broadcasted_iota(jnp.int32, (rows, rows), 1), xg)
        cbias[xg] = jnp.where(key_order <= query_order, 0.0, HIDDEN)
    for c in local:
        c.wait()
    for c in cross:
        c.wait_recv()
    block = 512
    for j in range(RING):
        for b in range(cached // block):
            vt[j, :, pl.ds(b * block, block)] = vbuf[j, pl.ds(b * block, block)].T
        vt[j, :, tail] = vbuf[j, tail].T

    def p1(g, i, src, dst, target):
        return remote(src, dst, ps.at[g, i], pr.at[g, i], target)

    def send_a(g):
        far, near_up, near_down = ring(a1 + 2), ring(a1 + 1), ring(a1 - 1)
        return (
            p1(g, 0, ob.at[g, far, two_lo], r1.at[g, 0], on1(1)),
            p1(g, 1, ob.at[g, far, two_hi], r1.at[g, 1], on1(-1)),
            p1(g, 2, ob.at[g, near_up, two_hi], n1.at[g, 0, two_hi], on1(1)),
            p1(g, 3, ob.at[g, near_down, two_lo], n1.at[g, 1, two_lo], on1(-1)),
            p1(g, 4, ob.at[g, near_up, two_lo], n1.at[g, 0, two_lo], on1(1)),
            p1(g, 5, ob.at[g, near_down, two_hi], n1.at[g, 1, two_hi], on1(-1)),
        )

    def send_b(g):
        d = 1 - 2 * lax.rem(g, 2)
        return (
            p1(g, 6, ob.at[g, a1, ring(a2 + 2)], r2.at[g], on2(d)),
            p1(g, 7, ob.at[g, a1, ring(a2 - d)], n2.at[g, 0], on2(-d)),
            p1(g, 8, ob.at[g, a1, ring(a2 + d)], n2.at[g, 1], on2(d)),
        )

    def reduce_start(g):
        for c in send_a(g)[:4]:
            c.start()

    def reduce_1(g):
        copies = send_a(g)
        for i in range(2):
            copies[i].wait_recv()
            to = ring(a1 + 1 - 2 * i)
            for b in range(2):
                put_block(ob, (g, to, 2 * i + b), *merge([ob[g, to, 2 * i + b], r1[g, i, b]]))
            copies[4 + i].start()

    def reduce_2(g):
        copies = send_a(g)
        for i in range(2, 6):
            copies[i].wait_recv()
        for b in range(RING):
            put_block(ob, (g, a1, b), *merge([ob[g, a1, b], n1[g, 0, b], n1[g, 1, b]]))
        copies = send_b(g)
        copies[0].start()
        copies[1].start()

    def reduce_3(g):
        copies = send_b(g)
        copies[0].wait_recv()
        to = ring(a2 + 1 - 2 * lax.rem(g, 2))
        put_block(ob, (g, a1, to), *merge([ob[g, a1, to], r2[g]]))
        copies[2].start()

    def reduce_4(g):
        copies = send_b(g)
        copies[1].wait_recv()
        copies[2].wait_recv()
        total, _, norm = merge([ob[g, a1, a2], n2[g, 0], n2[g, 1]])
        ox[g] = (total / norm).T.astype(jnp.bfloat16)

    q2_relay(0)

    @pl.loop(0, heads * 2 * RING)
    def _(u):
        g, t, part = u // (2 * RING), lax.rem(u // 2, RING), lax.rem(u, 2)

        @pl.when(lax.rem(u, 2 * RING) == 0)
        def _():
            q2_done(g)

        places = []
        for i in range(2):
            xg = 2 * part + i
            places.append((xg + core * (t - xg), t + core * (xg - t)))
        q = jnp.concatenate([qbuf[g, p2, p1_] for p1_, p2 in places], axis=0)
        top = None
        for b in range(cached // block):
            at = pl.ds(b * block, block)
            mask = bias[at]
            s = dot_nt(kbuf[t, at], q) + jnp.concatenate([mask, mask], axis=1)
            sbuf[at] = s
            here = jnp.max(s, axis=0, keepdims=True)
            top = here if top is None else jnp.maximum(top, here)
        unseen = jnp.where(t == y, 0.0, HIDDEN)
        s = dot_nt(kbuf[t, tail], q) + jnp.concatenate([cbias[2 * part], cbias[2 * part + 1]], axis=1) + unseen
        sbuf[tail] = s
        top = jnp.maximum(top, jnp.max(s, axis=0, keepdims=True)) * SCALE2
        norm, total = 0.0, 0.0
        for at in [pl.ds(b * block, block) for b in range(cached // block)] + [tail]:
            e = jnp.exp2(sbuf[at] * SCALE2 - top)
            norm = norm + jnp.sum(e, axis=0, keepdims=True)
            total = total + dot(vt[t, :, at], e.astype(jnp.bfloat16))
        for i, (p1_, p2) in enumerate(places):
            cut = slice(i * rows, (i + 1) * rows)
            put_block(ob, (g, p1_, p2), total[:, cut], top[:, cut], norm[:, cut])

        r = lax.rem(u, 2 * RING)
        for g_next in range(1, heads):
            @pl.when(u == 2 * g_next)
            def _():
                q2_relay(g_next)

        @pl.when(r == 2 * RING - 1)
        def _():
            reduce_start(g)

        for at, step in ((2, reduce_1), (4, reduce_2), (5, reduce_3), (6, reduce_4)):
            @pl.when(jnp.logical_and(r == at, g > 0))
            def _():
                step(g - 1)

    for step in (reduce_1, reduce_2, reduce_3, reduce_4):
        step(heads - 1)

    keep = pl.ds(pl.multiple_of(core * (rows // 2), rows // 2), rows // 2)
    give = pl.ds(pl.multiple_of(other * (rows // 2), rows // 2), rows // 2)
    swap = remote(ox.at[:, give], oin, os_, or_, sibling)
    swap.start()
    o_ref[core] = ox[:, keep]
    swap.wait()
    o_ref[other] = oin[...]
    for c in cross:
        c.wait_send()
    for g in range(heads):
        for c in (q1(g, 0, a1, None, on1(1)), q1(g, 1, a1, None, on1(1)), q1(g, 2, a1, lo, on1(1)), q1(g, 3, a1, hi, on1(1))):
            c.wait_send()
        for c in (q2(g, 4, a2, None, on2(1)), q2(g, 5, a2, None, on2(1)), q2(g, 6, a2, two_lo, on2(1)), q2(g, 7, a2, two_hi, on2(1))):
            c.wait_send()
        for c in (*send_a(g), *send_b(g)):
            c.wait_send()


def attend(cache_len, q, k_new, v_new, cache_k, cache_v):
    heads, rows, _ = q.shape
    slots = cache_k.shape[0]
    total = 2 * slots + rows
    bf16, f32 = jnp.bfloat16, jnp.float32
    deep = HEAD_DIM + 8
    vmem, hbm, smem = pl.BlockSpec(memory_space=pltpu.VMEM), pl.BlockSpec(memory_space=pl.ANY), pl.BlockSpec(memory_space=pltpu.SMEM)
    dma = pltpu.SemaphoreType.DMA
    return pl.pallas_call(
        attend_kernel,
        out_shape=jax.ShapeDtypeStruct((2, heads, rows // 2, HEAD_DIM), bf16),
        in_specs=[smem, vmem, vmem, vmem, hbm, hbm],
        out_specs=vmem,
        scratch_shapes=[
            pltpu.VMEM((RING, total, HEAD_DIM), bf16),
            pltpu.VMEM((RING, total, HEAD_DIM), bf16),
            pltpu.VMEM((RING, HEAD_DIM, total), bf16),
            pltpu.VMEM((heads, RING, RING, rows, HEAD_DIM), bf16),
            pltpu.VMEM((2 * slots, HEAD_DIM), f32),
            pltpu.VMEM((RING, rows, rows), f32),
            pltpu.VMEM((total, 2 * rows), f32),
            pltpu.VMEM((heads, RING, RING, deep, rows), f32),
            pltpu.VMEM((heads, 2, 2, deep, rows), f32),
            pltpu.VMEM((heads, 2, RING, deep, rows), f32),
            pltpu.VMEM((heads, deep, rows), f32),
            pltpu.VMEM((heads, 2, deep, rows), f32),
            pltpu.VMEM((heads, rows, HEAD_DIM), bf16),
            pltpu.VMEM((heads, rows // 2, HEAD_DIM), bf16),
            dma((2 * RING,)),
            dma((2 * RING,)),
            dma((2 * RING,)),
            dma((heads, 8)),
            dma((heads, 8)),
            dma((heads, 9)),
            dma((heads, 9)),
            dma,
            dma,
        ],
        compiler_params=pltpu.CompilerParams(collective_id=1, has_side_effects=True, vmem_limit_bytes=VMEM_LIMIT),
    )(cache_len, q, k_new, v_new, cache_k, cache_v)


def mlp_kernel(o_in, x_ref, gain_ref, wo_hbm, wg_hbm, wu_hbm, wd_hbm, out_ref, wo, wg, wu, wd, part, far, near, mid, rows, act, wsem, ss, rs):
    x, y, core = place()
    shard_rows, width = x_ref.shape
    all_rows = RING * shard_rows
    half = width // 2
    loads = [pltpu.make_async_copy(src, dst, wsem.at[i]) for i, (src, dst) in enumerate(((wo_hbm, wo), (wg_hbm, wg), (wu_hbm, wu), (wd_hbm, wd)))]
    for load in loads:
        load.start()
    up, down = device(x, y + 1, core), device(x, y - 1, core)
    greet((up, down))
    lo, hi = pl.ds(0, half), pl.ds(half, half)
    pending = []

    def reduce_rows(n):
        def copy(i, src, dst, target):
            return remote(src, dst, ss.at[n, i], rs.at[n, i], target)

        copies = (
            copy(0, part.at[ring(y + 2), :, lo], far.at[n, 0], up),
            copy(1, part.at[ring(y + 2), :, hi], far.at[n, 1], down),
            copy(2, part.at[ring(y + 1), :, hi], near.at[n, 0, :, hi], up),
            copy(3, part.at[ring(y - 1), :, lo], near.at[n, 1, :, lo], down),
            copy(4, part.at[ring(y + 1), :, lo], near.at[n, 0, :, lo], up),
            copy(5, part.at[ring(y - 1), :, hi], near.at[n, 1, :, hi], down),
        )
        for c in copies[:4]:
            c.start()
        copies[0].wait_recv()
        part[ring(y + 1), :, lo] = part[ring(y + 1), :, lo] + far[n, 0]
        copies[4].start()
        copies[1].wait_recv()
        part[ring(y - 1), :, hi] = part[ring(y - 1), :, hi] + far[n, 1]
        copies[5].start()
        for c in copies[2:]:
            c.wait_recv()
        total = part[y] + (near[n, 0] + near[n, 1])
        for c in copies:
            c.wait_send()
        return total

    o = jnp.concatenate([o_in[c, g] for c in range(2) for g in range(o_in.shape[1])], axis=1)
    loads[0].wait()
    cols = 768

    @pl.loop(0, width // cols)
    def _(i):
        at = pl.ds(pl.multiple_of(i * cols, cols), cols)
        part[:, :, at] = dot(o, wo[:, at]).reshape(RING, shard_rows, cols)

    h = (x_ref[...].astype(jnp.float32) + reduce_rows(0)).astype(jnp.bfloat16)
    mid[...] = h
    rows[y] = normalize(h.astype(jnp.float32), gain_ref[...])

    def copy(i, block, cut, target):
        ref = rows.at[ring(block)] if cut is None else rows.at[ring(block), :, cut]
        return remote(ref, ref, ss.at[2, i], rs.at[2, i], target)

    sends = [copy(0, y, None, up), copy(1, y, None, down)]
    for c in sends:
        c.start()
    copy(0, y - 1, None, up).wait_recv()
    sends.append(copy(2, y - 1, lo, up))
    sends[-1].start()
    copy(1, y + 1, None, up).wait_recv()
    sends.append(copy(3, y + 1, hi, down))
    sends[-1].start()
    copy(2, y - 2, lo, up).wait_recv()
    copy(3, y + 2, hi, up).wait_recv()
    b = rows[...].reshape(all_rows, width)
    loads[1].wait()
    loads[2].wait()
    wide = 512

    @pl.loop(0, act.shape[1] // wide)
    def _(i):
        at = pl.ds(pl.multiple_of(i * wide, wide), wide)
        gate = dot(b, wg[:, at])
        act[:, at] = (gate * jax.nn.sigmoid(gate) * dot(b, wu[:, at])).astype(jnp.bfloat16)

    loads[3].wait()
    a = act[...]

    @pl.loop(0, width // cols)
    def _(i):
        at = pl.ds(pl.multiple_of(i * cols, cols), cols)
        part[:, :, at] = dot(a, wd[:, at]).reshape(RING, shard_rows, cols)

    out_ref[...] = (mid[...].astype(jnp.float32) + reduce_rows(1)).astype(jnp.bfloat16)
    for c in sends:
        c.wait_send()


def mlp(o, hidden, gain, w_out, w_gate, w_up, w_down):
    shard_rows, width = hidden.shape
    inner = w_gate.shape[1]
    bf16, f32 = jnp.bfloat16, jnp.float32
    vmem, hbm = pl.BlockSpec(memory_space=pltpu.VMEM), pl.BlockSpec(memory_space=pl.ANY)
    dma = pltpu.SemaphoreType.DMA
    return pl.pallas_call(
        mlp_kernel,
        out_shape=jax.ShapeDtypeStruct(hidden.shape, bf16),
        in_specs=[vmem, vmem, vmem, hbm, hbm, hbm, hbm],
        out_specs=vmem,
        scratch_shapes=[
            pltpu.VMEM(w_out.shape, bf16),
            pltpu.VMEM(w_gate.shape, bf16),
            pltpu.VMEM(w_up.shape, bf16),
            pltpu.VMEM(w_down.shape, bf16),
            pltpu.VMEM((RING, shard_rows, width), f32),
            pltpu.VMEM((2, 2, shard_rows, width // 2), f32),
            pltpu.VMEM((2, 2, shard_rows, width), f32),
            pltpu.VMEM((shard_rows, width), bf16),
            pltpu.VMEM((RING, shard_rows, width), bf16),
            pltpu.VMEM((RING * shard_rows, inner), bf16),
            dma((4,)),
            dma((3, 6)),
            dma((3, 6)),
        ],
        compiler_params=pltpu.CompilerParams(collective_id=2, has_side_effects=True, vmem_limit_bytes=VMEM_LIMIT),
    )(o, hidden, gain, w_out, w_gate, w_up, w_down)


def solution(mesh):
    devices = mesh.shape['tp'] * mesh.shape['cp']
    assert mesh.shape['tp'] == RING and mesh.shape['cp'] == 2 * RING
    token_spec = P(('dp', 'cp', 'tp'), None)
    column_spec = P(None, 'tp')
    row_spec = P('tp', None)

    def tables(cache_len, shard_rows):
        half_rows, half_dim = shard_rows // 2, HEAD_DIM // 2
        row = jnp.arange(2 * RING * shard_rows, dtype=jnp.int32)
        owner = (lax.axis_index('cp') // 2) * (2 * RING) + row // shard_rows
        r = row % shard_rows
        run = jnp.where(r < half_rows, owner, 2 * devices - 1 - owner)
        pos = cache_len[0] + run * half_rows + r % half_rows
        inv_freq = 1.0 / (ROPE_BASE ** (jnp.arange(half_dim, dtype=jnp.float32) * (2.0 / HEAD_DIM)))
        angles = pos.astype(jnp.float32)[:, None] * inv_freq[None, :]
        cos, sin = jnp.cos(angles), jnp.sin(angles)
        return jnp.concatenate([cos, cos], axis=1), jnp.concatenate([-sin, sin], axis=1)

    def device_layer(hidden, pos, cache_len, cache_k, cache_v, norm1_gain, w_query, w_key, w_value, w_out, norm2_gain, w_gate, w_up, w_down):
        cos, sin = tables(cache_len, hidden.shape[0])
        q, k_new, v_new = project(hidden, norm1_gain[None], w_query, w_key, w_value, cos, sin)
        o = attend(cache_len, q, k_new, v_new, cache_k, cache_v)
        return mlp(o, hidden, norm2_gain[None], w_out, w_gate, w_up, w_down)

    return jax.shard_map(device_layer, mesh=mesh, in_specs=(token_spec, P(('dp', 'cp', 'tp')), P('dp'), token_spec, token_spec, P(), column_spec, column_spec, column_spec, row_spec, P(), column_spec, column_spec, row_spec), out_specs=token_spec, check_vma=False)
```

```python
import functools
import math

import jax
import jax.numpy as jnp
from jax import lax
from jax.experimental import pallas as pl
from jax.experimental.pallas import tpu as pltpu
from jax.sharding import PartitionSpec as P

HEAD_DIM = 128
ROPE_BASE = 500000.0
NORM_EPS = 1e-5
HIDDEN = -1e38
SCALE2 = math.log2(math.e) / math.sqrt(HEAD_DIM)
MESH = pl.DeviceIdType.MESH
RING = 4
VMEM_LIMIT = 67_043_328


def place():
    c = lax.axis_index('cp')
    return c // 2, lax.axis_index('tp'), lax.rem(c, 2)


def ring(i):
    return lax.rem(i + RING, RING)


def device(x, y, core):
    return {'tp': ring(y), 'cp': 2 * ring(x) + core}


def remote(src, dst, send_sem, recv_sem, target):
    return pltpu.make_async_remote_copy(src_ref=src, dst_ref=dst, send_sem=send_sem, recv_sem=recv_sem, device_id=target, device_id_type=MESH)


def greet(partners):
    for partner in partners:
        pl.semaphore_signal(pltpu.get_barrier_semaphore(), inc=1, device_id=partner, device_id_type=MESH)


def normalize(values, gain):
    inv_rms = lax.rsqrt(jnp.mean(values * values, axis=-1, keepdims=True) + NORM_EPS)
    return (values * inv_rms * gain.astype(jnp.float32)).astype(jnp.bfloat16)


def dot(a, b):
    return jnp.dot(a, b, preferred_element_type=jnp.float32)


def dot_nt(a, b):
    return lax.dot_general(a, b, (((1,), (1,)), ((), ())), preferred_element_type=jnp.float32)


def merge(parts):
    top = parts[0][HEAD_DIM : HEAD_DIM + 1]
    for p in parts[1:]:
        top = jnp.maximum(top, p[HEAD_DIM : HEAD_DIM + 1])
    total, norm = 0.0, 0.0
    for p in parts:
        weight = jnp.exp2(p[HEAD_DIM : HEAD_DIM + 1] - top)
        total = total + p[:HEAD_DIM] * weight
        norm = norm + p[HEAD_DIM + 1 : HEAD_DIM + 2] * weight
    return total, top, norm


def put_block(ref, index, total, top, norm):
    ref[(*index, pl.ds(0, HEAD_DIM))] = total
    ref[(*index, pl.ds(HEAD_DIM, 8))] = jnp.concatenate([top, norm, jnp.zeros((6, total.shape[1]), jnp.float32)], axis=0)


def layer_kernel(
    len_ref, x_ref, gain1_ref, gain2_ref, cos_ref, sin_ref, ck_hbm, cv_hbm, wq_hbm, wk_hbm, wv_hbm, wo_hbm, wg_hbm, wu_hbm, wd_hbm, out_ref,
    a_rows, knew, vnew, vt, qbuf, bias, cbias, ob, r1, n1, r2, n2, ox, oin, obuf, sbuf_a, sbuf_b, top_a, top_b, wo, wg, wu, wd, part, far, near, mid, b_rows, act,
    load_sem, csem, xs, xr, as_, ar, fs, fr, bs, br, gs, gr, ps, pr, ts, tr, os_, or_, wsem, ss, rs,
):
    x, y, core = place()
    other = 1 - core
    shard_rows, width = x_ref.shape
    heads = qbuf.shape[0]
    slots = ck_hbm.shape[0]
    cached = 2 * slots
    rows = qbuf.shape[3]
    half_rows = shard_rows // 2
    half = width // 2
    tail = pl.ds(cached, rows)
    lo, hi = pl.ds(0, half), pl.ds(half, half)
    a1, a2 = x + core * (y - x), y + core * (x - y)
    sibling, up, down = device(x, y, other), device(x, y + 1, core), device(x, y - 1, core)

    def on1(d):
        return device(x + d * other, y + d * core, core)

    def on2(d):
        return device(x + d * core, y + d * other, core)

    mine = pl.ds(pl.multiple_of(core * slots, slots), slots)

    def head_cols(j, c):
        return pl.ds(pl.multiple_of((2 * j + c) * HEAD_DIM, HEAD_DIM), HEAD_DIM)

    def kept(j, i):
        return wd.at[mine, pl.ds((RING * (1 - i) + j) * HEAD_DIM, HEAD_DIM)]

    local = [pltpu.make_async_copy(src.at[:, head_cols(j, core)], kept(j, i), csem.at[2 * j + i]) for j in range(RING) for i, src in enumerate((ck_hbm, cv_hbm))]
    cross = [remote(src.at[:, head_cols(j, other)], kept(j, i), xs.at[2 * j + i], xr.at[2 * j + i], sibling) for j in range(RING) for i, src in enumerate((ck_hbm, cv_hbm))]
    weights = [pltpu.make_async_copy(src, dst, wsem.at[i]) for i, (src, dst) in enumerate(((wo_hbm, wo), (wg_hbm, wg), (wu_hbm, wu)))]

    def order(i, xg):
        c_part, rest = i // (rows // 2), lax.rem(i, rows // 2)
        t_part, r = rest // shard_rows, lax.rem(rest, shard_rows)
        owner = (2 * xg + c_part) * RING + t_part
        run = jnp.where(r < half_rows, owner, 4 * RING * RING - 1 - owner)
        return run * half_rows + lax.rem(r, half_rows)

    def masks():
        length = len_ref[0]
        for piece in range(2):
            base = ((2 * x + piece) * RING + y) * slots
            slot = base + lax.broadcasted_iota(jnp.int32, (slots, HEAD_DIM), 0)
            lane = lax.broadcasted_iota(jnp.int32, (slots, HEAD_DIM), 1)
            bias[pl.ds(piece * slots, slots)] = jnp.where(jnp.logical_and(slot >= length, lane == 0), HIDDEN, 0.0).astype(jnp.bfloat16)
        key_order = order(lax.broadcasted_iota(jnp.int32, (rows, rows), 0), x)
        for xg in range(RING):
            query_order = order(lax.broadcasted_iota(jnp.int32, (rows, rows), 1), xg)
            cbias[xg] = jnp.where(key_order <= query_order, 0.0, HIDDEN)

    two_lo, two_hi = pl.ds(0, 2), pl.ds(2, 2)

    def q1(g):
        ref = qbuf.at[g, a2, a1]
        return [remote(ref, ref, gs.at[g, i], gr.at[g, i], on1(d)) for i, d in enumerate((2, 1, -1))]

    def q2(g, i):
        d, index, piece, to = ((0, 0, two_lo, 1), (1, 0, two_hi, -1), (2, 0, two_hi, 1), (3, 0, two_lo, -1), (4, -1, two_lo, 1), (5, 1, two_hi, -1))[i]
        ref = qbuf.at[g, ring(a2 + index), piece]
        return remote(ref, ref, gs.at[g, 3 + i], gr.at[g, 3 + i], on2(to))

    def q1_done(g):
        for c in q1(g):
            c.wait_recv()
        for i in range(4):
            q2(g, i).start()

    def q2_relay(g):
        for i in range(2):
            q2(g, i).wait_recv()
            q2(g, 4 + i).start()

    def q2_early(g):
        q2(g, 3).wait_recv()

    def q2_late(g):
        for i in (2, 4, 5):
            q2(g, i).wait_recv()

    pending = []

    def go(c):
        c.start()
        pending.append(c)
        return c

    block = 512

    def turn(j):
        for b in range(cached // block):
            vt[j, :, pl.ds(b * block, block)] = wd[pl.ds(b * block, block), pl.ds(j * HEAD_DIM, HEAD_DIM)].T

    def gather(block, sends, recvs, seen):
        hops = ((0, lo, up), (0, hi, down), (0, hi, up), (0, lo, down), (-1, lo, up), (1, hi, down))
        arrivals = ((-1, lo), (1, hi), (-1, hi), (1, lo), (-2, lo), (2, hi))

        def hop(n):
            d, cols, to = hops[n]
            return remote(block(y + d, cols), block(y + d, cols), sends.at[n], recvs.at[n], to)

        for n in range(4):
            go(hop(n))
        for n, (d, cols) in enumerate(arrivals):
            hop(n).wait_recv()
            if n < 2:
                go(hop(4 + n))
            seen(n, block(y + d, cols), cols)

    loads = []
    wide = heads * HEAD_DIM
    for i, (src, w, at) in enumerate(((wq_hbm, wide, 0), (wk_hbm, HEAD_DIM, wide), (wv_hbm, HEAD_DIM, wide + HEAD_DIM))):
        loads.append(pltpu.make_async_copy(src.at[:, pl.ds(pl.multiple_of(core * w, w), w)], wg.at[:, pl.ds(at, w)], load_sem.at[i]))
        loads[-1].start()
    for c in local:
        c.start()
    partners = (sibling, on1(1), on1(-1), on2(1), on2(-1), on1(2))
    greet(partners)
    a_rows[core, y] = normalize(x_ref[...].astype(jnp.float32), gain1_ref[...].reshape(1, width))
    pl.semaphore_wait(pltpu.get_barrier_semaphore(), len(partners))
    whole = pl.ds(0, width)

    def row_block(c):
        return lambda i, cols: a_rows.at[c, ring(i), :, cols]

    def forward(n, block, cols):
        go(remote(block, block, fs.at[n], fr.at[n], sibling))

    own = row_block(core)(y, whole)
    go(remote(own, own, fs.at[6], fr.at[6], sibling))
    for c in cross:
        c.start()
    gather(row_block(core), as_, ar, forward)
    for n, (d, cols) in enumerate(((-1, lo), (1, hi), (-1, hi), (1, lo), (-2, lo), (2, hi), (0, whole))):
        ref = row_block(other)(y + d, cols)
        remote(ref, ref, fs.at[n], fr.at[n], sibling).wait_recv()
    for load in loads:
        load.wait()
    a = a_rows[...].reshape(rows, width)
    cos, sin = cos_ref[...], sin_ref[...]

    def rotate(p):
        return (p * cos + pltpu.roll(p, HEAD_DIM // 2, axis=1) * sin).astype(jnp.bfloat16)

    q = dot(a, wg[:, :wide])
    for g in range(heads):
        qbuf[g, a2, a1] = rotate(q[:, g * HEAD_DIM : (g + 1) * HEAD_DIM])
        for c in q1(g):
            c.start()
    knew[...] = rotate(dot(a, wg[:, wide : wide + HEAD_DIM]))
    vnew[...] = dot(a, wg[:, wide + HEAD_DIM : wide + 2 * HEAD_DIM]).T.astype(jnp.bfloat16)
    for w in weights:
        w.start()
    masks()
    for i in range(2 * RING):
        local[i].wait()
        cross[i].wait_recv()
    turn(0)
    for g in range(heads):
        q1_done(g)
    for j in range(1, RING):
        turn(j)

    def granule(g, h):
        flip = (g + 1) // heads
        back = h + flip - 2 * flip * h
        return ring(a2 - back), ring(a2 + 1 + back)

    def first(g, h):
        far, near_up, near_down = ring(a1 + 2), ring(a1 + 1), ring(a1 - 1)
        even, odd = granule(g, h)

        def hop(i, src, dst, target):
            return remote(src, dst, ps.at[g, h, i], pr.at[g, h, i], target)

        return (
            lambda: hop(0, ob.at[g, far, even], r1.at[g, h, 0], on1(1)),
            lambda: hop(1, ob.at[g, far, odd], r1.at[g, h, 1], on1(-1)),
            lambda: hop(2, ob.at[g, near_up, odd], n1.at[g, 0, odd], on1(1)),
            lambda: hop(3, ob.at[g, near_down, even], n1.at[g, 1, even], on1(-1)),
            lambda: hop(4, ob.at[g, near_up, even], n1.at[g, 0, even], on1(1)),
            lambda: hop(5, ob.at[g, near_down, odd], n1.at[g, 1, odd], on1(-1)),
        )

    def second(g):
        d = 1 - 2 * lax.rem(g, 2)

        def hop(i, src, dst, target):
            return remote(src, dst, ts.at[g, i], tr.at[g, i], target)

        return (
            lambda: hop(0, ob.at[g, a1, ring(a2 + 2)], r2.at[g], on2(d)),
            lambda: hop(1, ob.at[g, a1, ring(a2 - d)], n2.at[g, 0], on2(-d)),
            lambda: hop(2, ob.at[g, a1, ring(a2 + d)], n2.at[g, 1], on2(d)),
        )

    def reduce_0(g, h):
        for c in first(g, h)[:4]:
            c().start()

    def reduce_1(g, h):
        copies = first(g, h)
        for i, b in enumerate(granule(g, h)):
            copies[i]().wait_recv()
            to = ring(a1 + 1 - 2 * i)
            put_block(ob, (g, to, b), *merge([ob[g, to, b], r1[g, h, i]]))
            copies[4 + i]().start()

    def reduce_2(g, h):
        copies = first(g, h)
        for i in range(2, 6):
            copies[i]().wait_recv()
        for b in granule(g, h):
            put_block(ob, (g, a1, b), *merge([ob[g, a1, b], n1[g, 0, b], n1[g, 1, b]]))

    def reduce_3(g):
        copies = second(g)
        copies[0]().start()
        copies[1]().start()

    def reduce_4(g):
        copies = second(g)
        copies[0]().wait_recv()
        to = ring(a2 + 1 - 2 * lax.rem(g, 2))
        put_block(ob, (g, a1, to), *merge([ob[g, a1, to], r2[g]]))
        copies[2]().start()

    def reduce_5(g):
        copies = second(g)
        copies[1]().wait_recv()
        copies[2]().wait_recv()
        total, _, norm = merge([ob[g, a1, a2], n2[g, 0], n2[g, 1]])
        ox[g] = (total / norm).T.astype(jnp.bfloat16)

    def unit(u):
        g, h, i = u // 8, lax.rem(u // 4, 2), lax.rem(u, 4)
        near, far_off = granule(g, h)
        t = (near + (i // 2) * (far_off - near)) * other + i * core
        pair = [(2 * lax.rem(i, 2) + n) * other + (near, far_off)[n] * core for n in range(2)]
        places = [(g, xg + core * (t - xg), t + core * (xg - t)) for xg in pair]
        return t, pair, places

    step = 512
    chunks = [pl.ds(b * step, step) for b in range(cached // step)] + [tail]

    def keys_at(t):
        return pl.ds(pl.multiple_of((RING + t) * HEAD_DIM, HEAD_DIM), HEAD_DIM)

    def advance(ahead, s_out, top_out, u, s_in, top_in):
        if ahead is not None:
            t_next, pair, q_places = unit(ahead)
            q = jnp.concatenate([qbuf[g, p2, p1] for g, p1, p2 in q_places], axis=0)
            unit_col = jnp.where(lax.broadcasted_iota(jnp.int32, q.shape, 1) == 0, 1.0, 0.0).astype(jnp.bfloat16)
            deep_q = jnp.concatenate([q, unit_col], axis=1)
            unseen = jnp.where(t_next == y, 0.0, HIDDEN)
            peak = jnp.full((8, 2 * rows), -jnp.inf, jnp.float32)
        if u is not None:
            t, _, places = unit(u)
            top = top_in[...]
            norm, total = jnp.zeros((8, 2 * rows), jnp.float32), 0.0
        for at in chunks:
            if ahead is not None:
                if at is tail:
                    s = dot_nt(knew[...], q) + (jnp.concatenate([cbias[xg] for xg in pair], axis=1) + unseen)
                else:
                    s = dot_nt(jnp.concatenate([wd[at, keys_at(t_next)], bias[at]], axis=1), deep_q)
                s_out[at] = s
                peak = jnp.maximum(peak, jnp.max(s.reshape(-1, 8, 2 * rows), axis=0))
            if u is not None:
                e = jnp.exp2(s_in[at] * SCALE2 - top)
                norm = norm + jnp.sum(e.reshape(-1, 8, 2 * rows), axis=0)
                total = total + dot(vnew[...] if at is tail else vt[t, :, at], e.astype(jnp.bfloat16))
        if ahead is not None:
            top_out[...] = jnp.max(peak, axis=0, keepdims=True) * SCALE2
        if u is not None:
            norm = jnp.sum(norm, axis=0, keepdims=True)
            for n, index in enumerate(places):
                cut = slice(n * rows, (n + 1) * rows)
                put_block(ob, index, total[:, cut], top[:, cut], norm[:, cut])

    q2_relay(0)
    q2_early(0)
    units = heads * 8
    advance(0, sbuf_a, top_a, None, None, None)

    @pl.loop(0, units // 2)
    def _(i):
        @pl.when(i == 1)
        def _():
            q2_late(0)

        for g in range(1, heads):
            @pl.when(i == 4 * g - 1)
            def _():
                q2_early(g)
                q2_late(g)

        u = 2 * i
        advance(u + 1, sbuf_b, top_b, u, sbuf_a, top_a)
        advance(jnp.minimum(u + 2, units - 1), sbuf_a, top_a, u + 1, sbuf_b, top_b)

        for g in range(1, heads):
            @pl.when(i == g - 1)
            def _():
                q2_relay(g)

        n = i // 2
        late = lax.rem(i, 2) == 1

        @pl.when(late)
        def _():
            reduce_0(n // 2, lax.rem(n, 2))

        @pl.when(jnp.logical_and(late, n >= 1))
        def _():
            reduce_1((n - 1) // 2, lax.rem(n - 1, 2))

        @pl.when(jnp.logical_and(late, n >= 2))
        def _():
            reduce_2((n - 2) // 2, lax.rem(n - 2, 2))

        for at, g, stage in [(4 * g + 7, g, reduce_3) for g in range(heads)] + [(4 * g + 9, g, reduce_4) for g in range(heads)] + [(4 * g + 11, g, reduce_5) for g in range(heads)]:
            if at < units // 2:
                @pl.when(i == at)
                def _():
                    stage(g)

    cols = width // RING

    sent = []

    def settle():
        while sent:
            sent.pop().wait_send()

    def reduce_rows(n, product):
        quarter = [pl.ds(i * cols, cols) for i in range(RING)]
        near_up, near_down = ring(y + 1), ring(y - 1)

        def hop(i, src, dst, target):
            return remote(src, dst, ss.at[n, i], rs.at[n, i], target)

        a_hops = [hop(i, part.at[ring(y + 2), :, q], far.at[n, :, q], up if i < 2 else down) for i, q in enumerate(quarter)]
        b_hops = [hop(4, part.at[near_up, :, hi], near.at[n, 0, :, hi], up), hop(5, part.at[near_down, :, lo], near.at[n, 1, :, lo], down)]
        c_hops = [hop(6 + i, part.at[near_up if i < 2 else near_down, :, q], near.at[n, i // 2, :, q], up if i < 2 else down) for i, q in enumerate(quarter)]
        turns = (0, 2, 1, 3)
        for i in turns:
            part[:, :, quarter[i]] = product(quarter[i]).reshape(RING, shard_rows, cols)
            a_hops[i].start()
        for c in b_hops:
            c.start()
        for i in turns:
            a_hops[i].wait_recv()
            to = near_up if i < 2 else near_down
            part[to, :, quarter[i]] = part[to, :, quarter[i]] + far[n, :, quarter[i]]
            c_hops[i].start()
        for c in b_hops + c_hops:
            c.wait_recv()
        sent.extend(a_hops + b_hops + c_hops)
        return part[y] + (near[n, 0] + near[n, 1])

    down_load = pltpu.make_async_copy(wd_hbm, wd, wsem.at[3])
    down_load.start()
    last = heads - 1
    reduce_1(last, 1)
    reduce_2(last, 0)
    reduce_3(last)
    reduce_4(last - 1)
    reduce_2(last, 1)
    reduce_4(last)
    reduce_5(last - 1)
    reduce_5(last)

    keep = pl.ds(pl.multiple_of(core * (rows // 2), rows // 2), rows // 2)
    give = pl.ds(pl.multiple_of(other * (rows // 2), rows // 2), rows // 2)
    swap = remote(ox.at[:, give], oin, os_, or_, sibling)
    swap.start()
    obuf[core] = ox[:, keep]
    swap.wait()
    obuf[other] = oin[...]
    o = jnp.concatenate([obuf[c, g] for c in range(2) for g in range(heads)], axis=1)
    weights[0].wait()
    h = (x_ref[...].astype(jnp.float32) + reduce_rows(0, lambda at: dot(o, wo[:, at]))).astype(jnp.bfloat16)
    mid[...] = h
    b_rows[y] = normalize(h.astype(jnp.float32), gain2_ref[...].reshape(1, width))

    gather(lambda i, cut: b_rows.at[ring(i), :, cut], bs, br, lambda *_: None)
    b = b_rows[...].reshape(RING * shard_rows, width)
    weights[1].wait()
    weights[2].wait()
    wide = act.shape[1] // 2

    @pl.loop(0, act.shape[1] // wide)
    def _(i):
        at = pl.ds(pl.multiple_of(i * wide, wide), wide)
        gate = dot(b, wg[:, at])
        act[:, at] = (gate * jax.nn.sigmoid(gate) * dot(b, wu[:, at])).astype(jnp.bfloat16)

    down_load.wait()
    inner = act[...]

    settle()
    out_ref[...] = (mid[...].astype(jnp.float32) + reduce_rows(1, lambda at: dot(inner, wd[:, at]))).astype(jnp.bfloat16)
    settle()
    for c in pending + cross:
        c.wait_send()
    for g in range(heads):
        for c in q1(g) + [q2(g, i) for i in range(6)]:
            c.wait_send()
        for c in (*first(g, 0), *first(g, 1), *second(g)):
            c().wait_send()


def layer(cache_len, hidden, gain1, gain2, cos, sin, cache_k, cache_v, w_query, w_key, w_value, w_out, w_gate, w_up, w_down):
    shard_rows, width = hidden.shape
    kv_local = w_key.shape[1] // HEAD_DIM
    heads = w_query.shape[1] // w_key.shape[1]
    rows = 2 * RING * shard_rows
    slots = cache_k.shape[0]
    total = 2 * slots + rows
    inner = w_gate.shape[1]
    deep = HEAD_DIM + 8
    assert kv_local == 2 and w_down.shape[0] >= 2 * slots and width >= 2 * RING * HEAD_DIM and inner >= (heads + 2) * HEAD_DIM and cache_k.shape[1] == 2 * RING * HEAD_DIM
    bf16, f32 = jnp.bfloat16, jnp.float32
    vmem, hbm, smem = pl.BlockSpec(memory_space=pltpu.VMEM), pl.BlockSpec(memory_space=pl.ANY), pl.BlockSpec(memory_space=pltpu.SMEM)
    dma = pltpu.SemaphoreType.DMA
    return pl.pallas_call(
        layer_kernel,
        out_shape=jax.ShapeDtypeStruct(hidden.shape, bf16),
        in_specs=[smem] + [vmem] * 5 + [hbm] * 9,
        out_specs=vmem,
        scratch_shapes=[
            pltpu.VMEM((2, RING, shard_rows, width), bf16),
            pltpu.VMEM((rows, HEAD_DIM), bf16),
            pltpu.VMEM((HEAD_DIM, rows), bf16),
            pltpu.VMEM((RING, HEAD_DIM, 2 * slots), bf16),
            pltpu.VMEM((heads, RING, RING, rows, HEAD_DIM), bf16),
            pltpu.VMEM((2 * slots, HEAD_DIM), bf16),
            pltpu.VMEM((RING, rows, rows), f32),
            pltpu.VMEM((heads, RING, RING, deep, rows), f32),
            pltpu.VMEM((heads, 2, 2, deep, rows), f32),
            pltpu.VMEM((heads, 2, RING, deep, rows), f32),
            pltpu.VMEM((heads, deep, rows), f32),
            pltpu.VMEM((heads, 2, deep, rows), f32),
            pltpu.VMEM((heads, rows, HEAD_DIM), bf16),
            pltpu.VMEM((heads, rows // 2, HEAD_DIM), bf16),
            pltpu.VMEM((2, heads, rows // 2, HEAD_DIM), bf16),
            pltpu.VMEM((total, 2 * rows), f32),
            pltpu.VMEM((total, 2 * rows), f32),
            pltpu.VMEM((1, 2 * rows), f32),
            pltpu.VMEM((1, 2 * rows), f32),
            pltpu.VMEM(w_out.shape, bf16),
            pltpu.VMEM(w_gate.shape, bf16),
            pltpu.VMEM(w_up.shape, bf16),
            pltpu.VMEM(w_down.shape, bf16),
            pltpu.VMEM((RING, shard_rows, width), f32),
            pltpu.VMEM((2, shard_rows, width), f32),
            pltpu.VMEM((2, 2, shard_rows, width), f32),
            pltpu.VMEM((shard_rows, width), bf16),
            pltpu.VMEM((RING, shard_rows, width), bf16),
            pltpu.VMEM((RING * shard_rows, inner), bf16),
            dma((3,)),
            dma((2 * RING,)),
            *(dma(shape) for shape in ((2 * RING,), (6,), (7,), (6,), (heads, 9), (heads, 2, 6), (heads, 3)) for _ in range(2)),
            dma,
            dma,
            dma((4,)),
            dma((2, 10)),
            dma((2, 10)),
        ],
        compiler_params=pltpu.CompilerParams(collective_id=0, has_side_effects=True, vmem_limit_bytes=VMEM_LIMIT),
        name='attend',
    )(cache_len, hidden, gain1, gain2, cos, sin, cache_k, cache_v, w_query, w_key, w_value, w_out, w_gate, w_up, w_down)


def solution(mesh):
    devices = mesh.shape['tp'] * mesh.shape['cp']
    assert mesh.shape['tp'] == RING and mesh.shape['cp'] == 2 * RING
    token_spec = P(('dp', 'cp', 'tp'), None)
    column_spec = P(None, 'tp')
    row_spec = P('tp', None)

    def tables(cache_len, shard_rows):
        half_rows, half_dim = shard_rows // 2, HEAD_DIM // 2
        row = jnp.arange(2 * RING * shard_rows, dtype=jnp.int32)
        owner = (lax.axis_index('cp') // 2) * (2 * RING) + row // shard_rows
        r = row % shard_rows
        run = jnp.where(r < half_rows, owner, 2 * devices - 1 - owner)
        pos = cache_len[0] + run * half_rows + r % half_rows
        inv_freq = 1.0 / (ROPE_BASE ** (jnp.arange(half_dim, dtype=jnp.float32) * (2.0 / HEAD_DIM)))
        angles = pos.astype(jnp.float32)[:, None] * inv_freq[None, :]
        cos, sin = jnp.cos(angles), jnp.sin(angles)
        return jnp.concatenate([cos, cos], axis=1), jnp.concatenate([-sin, sin], axis=1)

    def device_layer(hidden, pos, cache_len, cache_k, cache_v, norm1_gain, w_query, w_key, w_value, w_out, norm2_gain, w_gate, w_up, w_down):
        cos, sin = tables(cache_len, hidden.shape[0])
        return layer(cache_len, hidden, norm1_gain, norm2_gain, cos, sin, cache_k, cache_v, w_query, w_key, w_value, w_out, w_gate, w_up, w_down)

    return jax.shard_map(device_layer, mesh=mesh, in_specs=(token_spec, P(('dp', 'cp', 'tp')), P('dp'), token_spec, token_spec, P(), column_spec, column_spec, column_spec, row_spec, P(), column_spec, column_spec, row_spec), out_specs=token_spec, check_vma=False)
```

```python
import functools
import math

import jax
import jax.numpy as jnp
from jax import lax
from jax.experimental import pallas as pl
from jax.experimental.pallas import tpu as pltpu
from jax.sharding import PartitionSpec as P

HEAD_DIM = 128
ROPE_BASE = 500000.0
NORM_EPS = 1e-5
HIDDEN = -1e38
SCALE2 = math.log2(math.e) / math.sqrt(HEAD_DIM)
MESH = pl.DeviceIdType.MESH
RING = 4
VMEM_LIMIT = 67_043_328


def place():
    c = lax.axis_index('cp')
    return c // 2, lax.axis_index('tp'), lax.rem(c, 2)


def ring(i):
    return lax.rem(i + RING, RING)


def device(x, y, core):
    return {'tp': ring(y), 'cp': 2 * ring(x) + core}


def remote(src, dst, send_sem, recv_sem, target):
    return pltpu.make_async_remote_copy(src_ref=src, dst_ref=dst, send_sem=send_sem, recv_sem=recv_sem, device_id=target, device_id_type=MESH)


def greet(partners):
    for partner in partners:
        pl.semaphore_signal(pltpu.get_barrier_semaphore(), inc=1, device_id=partner, device_id_type=MESH)


def normalize(values, gain):
    inv_rms = lax.rsqrt(jnp.mean(values * values, axis=-1, keepdims=True) + NORM_EPS)
    return (values * inv_rms * gain.astype(jnp.float32)).astype(jnp.bfloat16)


def dot(a, b):
    return jnp.dot(a, b, preferred_element_type=jnp.float32)


def dot_nt(a, b):
    return lax.dot_general(a, b, (((1,), (1,)), ((), ())), preferred_element_type=jnp.float32)


def merge(parts):
    top = parts[0][HEAD_DIM : HEAD_DIM + 1]
    for p in parts[1:]:
        top = jnp.maximum(top, p[HEAD_DIM : HEAD_DIM + 1])
    total, norm = 0.0, 0.0
    for p in parts:
        weight = jnp.exp2(p[HEAD_DIM : HEAD_DIM + 1] - top)
        total = total + p[:HEAD_DIM] * weight
        norm = norm + p[HEAD_DIM + 1 : HEAD_DIM + 2] * weight
    return total, top, norm


def put_block(ref, index, total, top, norm):
    ref[(*index, pl.ds(0, HEAD_DIM))] = total
    ref[(*index, pl.ds(HEAD_DIM, 8))] = jnp.concatenate([top, norm, jnp.zeros((6, total.shape[1]), jnp.float32)], axis=0)


def layer_kernel(
    len_ref, x_ref, gain1_ref, gain2_ref, cos_ref, sin_ref, ck_hbm, cv_hbm, wq_hbm, wk_hbm, wv_hbm, wo_hbm, wg_hbm, wu_hbm, wd_hbm, out_ref,
    a_rows, knew, vnew, vt, qbuf, bias, cbias, ob, r1, n1, r2, n2, ox, oin, obuf, sbuf_a, sbuf_b, top_a, top_b, wo, wg, wu, wd, part, far, near, mid, b_rows, act,
    load_sem, csem, xs, xr, as_, ar, fs, fr, bs, br, gs, gr, ps, pr, ts, tr, os_, or_, wsem, ss, rs,
):
    x, y, core = place()
    other = 1 - core
    shard_rows, width = x_ref.shape
    heads = qbuf.shape[0]
    slots = ck_hbm.shape[0]
    cached = 2 * slots
    rows = qbuf.shape[3]
    half_rows = shard_rows // 2
    half = width // 2
    tail = pl.ds(cached, rows)
    lo, hi = pl.ds(0, half), pl.ds(half, half)
    a1, a2 = x + core * (y - x), y + core * (x - y)
    sibling, up, down = device(x, y, other), device(x, y + 1, core), device(x, y - 1, core)

    def on1(d):
        return device(x + d * other, y + d * core, core)

    def on2(d):
        return device(x + d * core, y + d * other, core)

    mine = pl.ds(pl.multiple_of(core * slots, slots), slots)

    def head_cols(j, c):
        return pl.ds(pl.multiple_of((2 * j + c) * HEAD_DIM, HEAD_DIM), HEAD_DIM)

    def kept(j, i):
        return wd.at[mine, pl.ds((RING * (1 - i) + j) * HEAD_DIM, HEAD_DIM)]

    local = [pltpu.make_async_copy(src.at[:, head_cols(j, core)], kept(j, i), csem.at[2 * j + i]) for j in range(RING) for i, src in enumerate((ck_hbm, cv_hbm))]
    cross = [remote(src.at[:, head_cols(j, other)], kept(j, i), xs.at[2 * j + i], xr.at[2 * j + i], sibling) for j in range(RING) for i, src in enumerate((ck_hbm, cv_hbm))]
    weights = [pltpu.make_async_copy(src, dst, wsem.at[i]) for i, (src, dst) in enumerate(((wo_hbm, wo), (wg_hbm, wg), (wu_hbm, wu)))]

    def order(i, xg):
        c_part, rest = i // (rows // 2), lax.rem(i, rows // 2)
        t_part, r = rest // shard_rows, lax.rem(rest, shard_rows)
        owner = (2 * xg + c_part) * RING + t_part
        run = jnp.where(r < half_rows, owner, 4 * RING * RING - 1 - owner)
        return run * half_rows + lax.rem(r, half_rows)

    def masks():
        length = len_ref[0]
        for piece in range(2):
            base = ((2 * x + piece) * RING + y) * slots
            slot = base + lax.broadcasted_iota(jnp.int32, (slots, HEAD_DIM), 0)
            lane = lax.broadcasted_iota(jnp.int32, (slots, HEAD_DIM), 1)
            bias[pl.ds(piece * slots, slots)] = jnp.where(jnp.logical_and(slot >= length, lane == 0), HIDDEN, 0.0).astype(jnp.bfloat16)
        key_order = order(lax.broadcasted_iota(jnp.int32, (rows, rows), 0), x)
        for xg in range(RING):
            query_order = order(lax.broadcasted_iota(jnp.int32, (rows, rows), 1), xg)
            cbias[xg] = jnp.where(key_order <= query_order, 0.0, HIDDEN)

    two_lo, two_hi = pl.ds(0, 2), pl.ds(2, 2)

    def q1(g):
        ref = qbuf.at[g, a2, a1]
        return [remote(ref, ref, gs.at[g, i], gr.at[g, i], on1(d)) for i, d in enumerate((2, 1, -1))]

    def q2(g, i):
        d, index, piece, to = ((0, 0, two_lo, 1), (1, 0, two_hi, -1), (2, 0, two_hi, 1), (3, 0, two_lo, -1), (4, -1, two_lo, 1), (5, 1, two_hi, -1))[i]
        ref = qbuf.at[g, ring(a2 + index), piece]
        return remote(ref, ref, gs.at[g, 3 + i], gr.at[g, 3 + i], on2(to))

    def q1_done(g):
        for c in q1(g):
            c.wait_recv()
        for i in range(4):
            q2(g, i).start()

    def q2_relay(g):
        for i in range(2):
            q2(g, i).wait_recv()
            q2(g, 4 + i).start()

    def q2_early(g):
        q2(g, 3).wait_recv()

    def q2_late(g):
        for i in (2, 4, 5):
            q2(g, i).wait_recv()

    pending = []

    def go(c):
        c.start()
        pending.append(c)
        return c

    block = 512

    def turn(j):
        for b in range(cached // block):
            vt[j, :, pl.ds(b * block, block)] = wd[pl.ds(b * block, block), pl.ds(j * HEAD_DIM, HEAD_DIM)].T

    def gather(block, sends, recvs, seen):
        hops = ((0, lo, up), (0, hi, down), (0, hi, up), (0, lo, down), (-1, lo, up), (1, hi, down))
        arrivals = ((-1, lo), (1, hi), (-1, hi), (1, lo), (-2, lo), (2, hi))

        def hop(n):
            d, cols, to = hops[n]
            return remote(block(y + d, cols), block(y + d, cols), sends.at[n], recvs.at[n], to)

        for n in range(4):
            go(hop(n))
        for n, (d, cols) in enumerate(arrivals):
            hop(n).wait_recv()
            if n < 2:
                go(hop(4 + n))
            seen(n, block(y + d, cols), cols)

    loads = []
    wide = heads * HEAD_DIM
    for i, (src, w, at) in enumerate(((wq_hbm, wide, 0), (wk_hbm, HEAD_DIM, wide), (wv_hbm, HEAD_DIM, wide + HEAD_DIM))):
        loads.append(pltpu.make_async_copy(src.at[:, pl.ds(pl.multiple_of(core * w, w), w)], wg.at[:, pl.ds(at, w)], load_sem.at[i]))
        loads[-1].start()
    for c in local:
        c.start()
    partners = (sibling, *(on(d) for on in (on1, on2) for d in (1, -1, 2)))
    greet(partners)
    a_rows[core, y] = normalize(x_ref[...].astype(jnp.float32), gain1_ref[...].reshape(1, width))
    pl.semaphore_wait(pltpu.get_barrier_semaphore(), len(partners))
    whole = pl.ds(0, width)

    def row_block(c):
        return lambda i, cols: a_rows.at[c, ring(i), :, cols]

    def forward(n, block, cols):
        go(remote(block, block, fs.at[n], fr.at[n], sibling))
        if n == 1:
            for c in cross:
                c.start()

    own = row_block(core)(y, whole)
    go(remote(own, own, fs.at[6], fr.at[6], sibling))
    gather(row_block(core), as_, ar, forward)
    for n, (d, cols) in enumerate(((-1, lo), (1, hi), (-1, hi), (1, lo), (-2, lo), (2, hi), (0, whole))):
        ref = row_block(other)(y + d, cols)
        remote(ref, ref, fs.at[n], fr.at[n], sibling).wait_recv()
    for load in loads:
        load.wait()
    a = a_rows[...].reshape(rows, width)
    cos, sin = cos_ref[...], sin_ref[...]

    def rotate(p):
        return (p * cos + pltpu.roll(p, HEAD_DIM // 2, axis=1) * sin).astype(jnp.bfloat16)

    q = dot(a, wg[:, :wide])
    for g in range(heads):
        qbuf[g, a2, a1] = rotate(q[:, g * HEAD_DIM : (g + 1) * HEAD_DIM])
        for c in q1(g):
            c.start()
    knew[...] = rotate(dot(a, wg[:, wide : wide + HEAD_DIM]))
    vnew[...] = dot(a, wg[:, wide + HEAD_DIM : wide + 2 * HEAD_DIM]).T.astype(jnp.bfloat16)
    for w in weights:
        w.start()
    masks()
    for i in range(2 * RING):
        local[i].wait()
        cross[i].wait_recv()
    turn(0)
    for g in range(heads):
        q1_done(g)
    for j in range(1, RING):
        turn(j)

    def back(g, h):
        flip = (g + 1) // heads
        return h + flip - 2 * flip * h

    def granule(g, h):
        return ring(a2 - back(g, h)), ring(a2 + 1 + back(g, h))

    def first(g, h, straight=False):
        far, near_up, near_down = ring(a1 + 2), ring(a1 + 1), ring(a1 - 1)
        even, odd = granule(g, h)

        def hop(i, src, dst, target):
            return remote(src, dst, ps.at[g, h, i], pr.at[g, h, i], target)

        return (
            lambda: hop(0, ob.at[g, far, even], r1.at[g, h, 0], on1(2 if straight else 1)),
            lambda: hop(1, ob.at[g, far, odd], r1.at[g, h, 1], on1(2 if straight else -1)),
            lambda: hop(2, ob.at[g, near_up, odd], n1.at[g, 0, odd], on1(1)),
            lambda: hop(3, ob.at[g, near_down, even], n1.at[g, 1, even], on1(-1)),
            lambda: hop(4, ob.at[g, near_up, even], n1.at[g, 0, even], on1(1)),
            lambda: hop(5, ob.at[g, near_down, odd], n1.at[g, 1, odd], on1(-1)),
        )

    def second(g):
        def hop(i, d, dst):
            return lambda: remote(ob.at[g, a1, ring(a2 + d)], dst, ts.at[g, i], tr.at[g, i], on2(d))

        return hop(0, 2, r2.at[g]), hop(1, -1, n2.at[g, 0]), hop(2, 1, n2.at[g, 1])

    def swap(g):
        give = pl.ds(pl.multiple_of(other * (rows // 2), rows // 2), rows // 2)
        return remote(ox.at[g, give], oin.at[g], os_.at[g], or_.at[g], sibling)

    def reduce_0(g, h, straight):
        copies = first(g, h, straight)
        for c in copies if straight else copies[:4]:
            c().start()

    def reduce_1(g, h):
        copies = first(g, h)
        for i, b in enumerate(granule(g, h)):
            copies[i]().wait_recv()
            to = ring(a1 + 1 - 2 * i)
            put_block(ob, (g, to, b), *merge([ob[g, to, b], r1[g, h, i]]))
            copies[4 + i]().start()

    def reduce_2(g, h, straight=False):
        for c in first(g, h)[0 if straight else 2 :]:
            c().wait_recv()
        for i, b in enumerate(granule(g, h)):
            put_block(ob, (g, a1, b), *merge([ob[g, a1, b], n1[g, 0, b], n1[g, 1, b]] + ([r1[g, h, i]] if straight else [])))

        @pl.when(back(g, h) == 0)
        def _():
            second(g)[2]().start()

        @pl.when(back(g, h) == 1)
        def _():
            second(g)[0]().start()
            second(g)[1]().start()

    def reduce_3(g):
        for c in second(g):
            c().wait_recv()
        total, _, norm = merge([ob[g, a1, a2], n2[g, 0], n2[g, 1], r2[g]])
        ox[g] = (total / norm).T.astype(jnp.bfloat16)
        swap(g).start()

    def unit(u):
        g, h, i = u // 8, lax.rem(u // 4, 2), lax.rem(u, 4)
        near, far_off = granule(g, h)
        t = (near + (i // 2) * (far_off - near)) * other + i * core
        pair = [(2 * lax.rem(i, 2) + n) * other + (near, far_off)[n] * core for n in range(2)]
        places = [(g, xg + core * (t - xg), t + core * (xg - t)) for xg in pair]
        return t, pair, places

    step = 512
    chunks = [pl.ds(b * step, step) for b in range(cached // step)] + [tail]

    def keys_at(t):
        return pl.ds(pl.multiple_of((RING + t) * HEAD_DIM, HEAD_DIM), HEAD_DIM)

    def advance(ahead, s_out, top_out, u, s_in, top_in):
        if ahead is not None:
            t_next, pair, q_places = unit(ahead)
            q = jnp.concatenate([qbuf[g, p2, p1] for g, p1, p2 in q_places], axis=0)
            unit_col = jnp.where(lax.broadcasted_iota(jnp.int32, q.shape, 1) == 0, 1.0, 0.0).astype(jnp.bfloat16)
            deep_q = jnp.concatenate([q, unit_col], axis=1)
            unseen = jnp.where(t_next == y, 0.0, HIDDEN)
            peak = jnp.full((8, 2 * rows), -jnp.inf, jnp.float32)
        if u is not None:
            t, _, places = unit(u)
            top = top_in[...]
            norm, total = jnp.zeros((8, 2 * rows), jnp.float32), 0.0
        for at in chunks:
            if ahead is not None:
                if at is tail:
                    s = dot_nt(knew[...], q) + (jnp.concatenate([cbias[xg] for xg in pair], axis=1) + unseen)
                else:
                    s = dot_nt(jnp.concatenate([wd[at, keys_at(t_next)], bias[at]], axis=1), deep_q)
                s_out[at] = s
                peak = jnp.maximum(peak, jnp.max(s.reshape(-1, 8, 2 * rows), axis=0))
            if u is not None:
                e = jnp.exp2(s_in[at] * SCALE2 - top)
                norm = norm + jnp.sum(e.reshape(-1, 8, 2 * rows), axis=0)
                total = total + dot(vnew[...] if at is tail else vt[t, :, at], e.astype(jnp.bfloat16))
        if ahead is not None:
            top_out[...] = jnp.max(peak, axis=0, keepdims=True) * SCALE2
        if u is not None:
            norm = jnp.sum(norm, axis=0, keepdims=True)
            for n, index in enumerate(places):
                cut = slice(n * rows, (n + 1) * rows)
                put_block(ob, index, total[:, cut], top[:, cut], norm[:, cut])

    q2_relay(0)
    q2_early(0)
    units = heads * 8
    advance(0, sbuf_a, top_a, None, None, None)

    @pl.loop(0, units // 2)
    def _(i):
        @pl.when(i == 1)
        def _():
            q2_late(0)

        for g in range(1, heads):
            @pl.when(i == 4 * g - 1)
            def _():
                q2_early(g)
                q2_late(g)

        u = 2 * i
        advance(u + 1, sbuf_b, top_b, u, sbuf_a, top_a)
        advance(jnp.minimum(u + 2, units - 1), sbuf_a, top_a, u + 1, sbuf_b, top_b)

        for g in range(1, heads):
            @pl.when(i == g - 1)
            def _():
                q2_relay(g)

        n = i // 2
        late = lax.rem(i, 2) == 1

        @pl.when(jnp.logical_and(late, n < 2 * heads - 1))
        def _():
            reduce_0(n // 2, lax.rem(n, 2), False)

        @pl.when(jnp.logical_and(late, n == 2 * heads - 1))
        def _():
            reduce_0(heads - 1, 1, True)

        @pl.when(jnp.logical_and(late, n >= 1))
        def _():
            reduce_1((n - 1) // 2, lax.rem(n - 1, 2))

        @pl.when(jnp.logical_and(late, n >= 2))
        def _():
            reduce_2((n - 2) // 2, lax.rem(n - 2, 2))

        @pl.when(i == units // 2 - 1)
        def _():
            reduce_3(0)

    cols = width // RING
    sent = []

    def settle():
        while sent:
            sent.pop().wait_send()

    def reduce_rows(n, product):
        quarter = [pl.ds(i * cols, cols) for i in range(RING)]
        near_up, near_down = ring(y + 1), ring(y - 1)

        def hop(i, src, dst, target):
            return remote(src, dst, ss.at[n, i], rs.at[n, i], target)

        a_hops = [hop(i, part.at[ring(y + 2), :, q], far.at[n, :, q], up if i < 2 else down) for i, q in enumerate(quarter)]
        b_hops = [hop(4, part.at[near_up, :, hi], near.at[n, 0, :, hi], up), hop(5, part.at[near_down, :, lo], near.at[n, 1, :, lo], down)]
        c_hops = [hop(6 + i, part.at[near_up if i < 2 else near_down, :, q], near.at[n, i // 2, :, q], up if i < 2 else down) for i, q in enumerate(quarter)]
        turns = (0, 2, 1, 3)
        for i in turns:
            part[:, :, quarter[i]] = product(quarter[i]).reshape(RING, shard_rows, cols)
            a_hops[i].start()
        for c in b_hops:
            c.start()
        for i in turns:
            a_hops[i].wait_recv()
            to = near_up if i < 2 else near_down
            part[to, :, quarter[i]] = part[to, :, quarter[i]] + far[n, :, quarter[i]]
            c_hops[i].start()
        for c in b_hops + c_hops:
            c.wait_recv()
        sent.extend(a_hops + b_hops + c_hops)
        return part[y] + (near[n, 0] + near[n, 1])

    down_load = pltpu.make_async_copy(wd_hbm, wd, wsem.at[3])
    down_load.start()
    last = heads - 1
    reduce_2(last, 0)
    for g in range(1, last):
        reduce_3(g)
    reduce_2(last, 1, True)
    reduce_3(last)
    keep = pl.ds(pl.multiple_of(core * (rows // 2), rows // 2), rows // 2)
    obuf[core] = ox[:, keep]
    for g in range(heads):
        swap(g).wait_recv()
    obuf[other] = oin[...]
    o = jnp.concatenate([obuf[c, g] for c in range(2) for g in range(heads)], axis=1)
    weights[0].wait()
    h = (x_ref[...].astype(jnp.float32) + reduce_rows(0, lambda at: dot(o, wo[:, at]))).astype(jnp.bfloat16)
    mid[...] = h
    b_rows[y] = normalize(h.astype(jnp.float32), gain2_ref[...].reshape(1, width))

    gather(lambda i, cut: b_rows.at[ring(i), :, cut], bs, br, lambda *_: None)
    b = b_rows[...].reshape(RING * shard_rows, width)
    weights[1].wait()
    weights[2].wait()
    wide = act.shape[1] // 2

    @pl.loop(0, act.shape[1] // wide)
    def _(i):
        at = pl.ds(pl.multiple_of(i * wide, wide), wide)
        gate = dot(b, wg[:, at])
        act[:, at] = (gate * jax.nn.sigmoid(gate) * dot(b, wu[:, at])).astype(jnp.bfloat16)

    down_load.wait()
    inner = act[...]

    settle()
    out_ref[...] = (mid[...].astype(jnp.float32) + reduce_rows(1, lambda at: dot(inner, wd[:, at]))).astype(jnp.bfloat16)
    settle()
    for c in pending + cross:
        c.wait_send()
    for g in range(heads):
        for c in q1(g) + [q2(g, i) for i in range(6)]:
            c.wait_send()
        for c in (*first(g, 0), *first(g, 1), *second(g)):
            c().wait_send()
        swap(g).wait_send()


def layer(cache_len, hidden, gain1, gain2, cos, sin, cache_k, cache_v, w_query, w_key, w_value, w_out, w_gate, w_up, w_down):
    shard_rows, width = hidden.shape
    kv_local = w_key.shape[1] // HEAD_DIM
    heads = w_query.shape[1] // w_key.shape[1]
    rows = 2 * RING * shard_rows
    slots = cache_k.shape[0]
    total = 2 * slots + rows
    inner = w_gate.shape[1]
    deep = HEAD_DIM + 8
    assert kv_local == 2 and w_down.shape[0] >= 2 * slots and width >= 2 * RING * HEAD_DIM and inner >= (heads + 2) * HEAD_DIM and cache_k.shape[1] == 2 * RING * HEAD_DIM
    bf16, f32 = jnp.bfloat16, jnp.float32
    vmem, hbm, smem = pl.BlockSpec(memory_space=pltpu.VMEM), pl.BlockSpec(memory_space=pl.ANY), pl.BlockSpec(memory_space=pltpu.SMEM)
    dma = pltpu.SemaphoreType.DMA
    return pl.pallas_call(
        layer_kernel,
        out_shape=jax.ShapeDtypeStruct(hidden.shape, bf16),
        in_specs=[smem] + [vmem] * 5 + [hbm] * 9,
        out_specs=vmem,
        scratch_shapes=[
            pltpu.VMEM((2, RING, shard_rows, width), bf16),
            pltpu.VMEM((rows, HEAD_DIM), bf16),
            pltpu.VMEM((HEAD_DIM, rows), bf16),
            pltpu.VMEM((RING, HEAD_DIM, 2 * slots), bf16),
            pltpu.VMEM((heads, RING, RING, rows, HEAD_DIM), bf16),
            pltpu.VMEM((2 * slots, HEAD_DIM), bf16),
            pltpu.VMEM((RING, rows, rows), f32),
            pltpu.VMEM((heads, RING, RING, deep, rows), f32),
            pltpu.VMEM((heads, 2, 2, deep, rows), f32),
            pltpu.VMEM((heads, 2, RING, deep, rows), f32),
            pltpu.VMEM((heads, deep, rows), f32),
            pltpu.VMEM((heads, 2, deep, rows), f32),
            pltpu.VMEM((heads, rows, HEAD_DIM), bf16),
            pltpu.VMEM((heads, rows // 2, HEAD_DIM), bf16),
            pltpu.VMEM((2, heads, rows // 2, HEAD_DIM), bf16),
            pltpu.VMEM((total, 2 * rows), f32),
            pltpu.VMEM((total, 2 * rows), f32),
            pltpu.VMEM((1, 2 * rows), f32),
            pltpu.VMEM((1, 2 * rows), f32),
            pltpu.VMEM(w_out.shape, bf16),
            pltpu.VMEM(w_gate.shape, bf16),
            pltpu.VMEM(w_up.shape, bf16),
            pltpu.VMEM(w_down.shape, bf16),
            pltpu.VMEM((RING, shard_rows, width), f32),
            pltpu.VMEM((2, shard_rows, width), f32),
            pltpu.VMEM((2, 2, shard_rows, width), f32),
            pltpu.VMEM((shard_rows, width), bf16),
            pltpu.VMEM((RING, shard_rows, width), bf16),
            pltpu.VMEM((RING * shard_rows, inner), bf16),
            dma((3,)),
            dma((2 * RING,)),
            *(dma(shape) for shape in ((2 * RING,), (6,), (7,), (6,), (heads, 9), (heads, 2, 6), (heads, 3), (heads,)) for _ in range(2)),
            dma((4,)),
            dma((2, 10)),
            dma((2, 10)),
        ],
        compiler_params=pltpu.CompilerParams(collective_id=0, has_side_effects=True, vmem_limit_bytes=VMEM_LIMIT),
        name='attend',
    )(cache_len, hidden, gain1, gain2, cos, sin, cache_k, cache_v, w_query, w_key, w_value, w_out, w_gate, w_up, w_down)


def solution(mesh):
    devices = mesh.shape['tp'] * mesh.shape['cp']
    assert mesh.shape['tp'] == RING and mesh.shape['cp'] == 2 * RING
    token_spec = P(('dp', 'cp', 'tp'), None)
    column_spec = P(None, 'tp')
    row_spec = P('tp', None)

    def tables(cache_len, shard_rows):
        half_rows, half_dim = shard_rows // 2, HEAD_DIM // 2
        row = jnp.arange(2 * RING * shard_rows, dtype=jnp.int32)
        owner = (lax.axis_index('cp') // 2) * (2 * RING) + row // shard_rows
        r = row % shard_rows
        run = jnp.where(r < half_rows, owner, 2 * devices - 1 - owner)
        pos = cache_len[0] + run * half_rows + r % half_rows
        inv_freq = 1.0 / (ROPE_BASE ** (jnp.arange(half_dim, dtype=jnp.float32) * (2.0 / HEAD_DIM)))
        angles = pos.astype(jnp.float32)[:, None] * inv_freq[None, :]
        cos, sin = jnp.cos(angles), jnp.sin(angles)
        return jnp.concatenate([cos, cos], axis=1), jnp.concatenate([-sin, sin], axis=1)

    def device_layer(hidden, pos, cache_len, cache_k, cache_v, norm1_gain, w_query, w_key, w_value, w_out, norm2_gain, w_gate, w_up, w_down):
        cos, sin = tables(cache_len, hidden.shape[0])
        return layer(cache_len, hidden, norm1_gain, norm2_gain, cos, sin, cache_k, cache_v, w_query, w_key, w_value, w_out, w_gate, w_up, w_down)

    return jax.shard_map(device_layer, mesh=mesh, in_specs=(token_spec, P(('dp', 'cp', 'tp')), P('dp'), token_spec, token_spec, P(), column_spec, column_spec, column_spec, row_spec, P(), column_spec, column_spec, row_spec), out_specs=token_spec, check_vma=False)
```

```python
import functools
import math

import jax
import jax.numpy as jnp
from jax import lax
from jax.experimental import pallas as pl
from jax.experimental.pallas import tpu as pltpu
from jax.sharding import PartitionSpec as P

HEAD_DIM = 128
ROPE_BASE = 500000.0
NORM_EPS = 1e-5
HIDDEN = -1e38
SCALE2 = math.log2(math.e) / math.sqrt(HEAD_DIM)
MESH = pl.DeviceIdType.MESH
RING = 4
VMEM_LIMIT = 67_043_328


def place():
    c = lax.axis_index('cp')
    return c // 2, lax.axis_index('tp'), lax.rem(c, 2)


def ring(i):
    return lax.rem(i + RING, RING)


def device(x, y, core):
    return {'tp': ring(y), 'cp': 2 * ring(x) + core}


def remote(src, dst, send_sem, recv_sem, target):
    return pltpu.make_async_remote_copy(src_ref=src, dst_ref=dst, send_sem=send_sem, recv_sem=recv_sem, device_id=target, device_id_type=MESH)


def greet(partners):
    for partner in partners:
        pl.semaphore_signal(pltpu.get_barrier_semaphore(), inc=1, device_id=partner, device_id_type=MESH)


def normalize(values, gain):
    inv_rms = lax.rsqrt(jnp.mean(values * values, axis=-1, keepdims=True) + NORM_EPS)
    return (values * inv_rms * gain.astype(jnp.float32)).astype(jnp.bfloat16)


def dot(a, b):
    return jnp.dot(a, b, preferred_element_type=jnp.float32)


def dot_nt(a, b):
    return lax.dot_general(a, b, (((1,), (1,)), ((), ())), preferred_element_type=jnp.float32)


def merge(parts):
    top = parts[0][HEAD_DIM : HEAD_DIM + 1]
    for p in parts[1:]:
        top = jnp.maximum(top, p[HEAD_DIM : HEAD_DIM + 1])
    total, norm = 0.0, 0.0
    for p in parts:
        weight = jnp.exp2(p[HEAD_DIM : HEAD_DIM + 1] - top)
        total = total + p[:HEAD_DIM] * weight
        norm = norm + p[HEAD_DIM + 1 : HEAD_DIM + 2] * weight
    return total, top, norm


def put_block(ref, index, total, top, norm):
    ref[(*index, pl.ds(0, HEAD_DIM))] = total
    ref[(*index, pl.ds(HEAD_DIM, 8))] = jnp.concatenate([top, norm, jnp.zeros((6, total.shape[1]), jnp.float32)], axis=0)


def layer_kernel(
    len_ref, x_ref, gain1_ref, gain2_ref, cos_ref, sin_ref, ck_hbm, cv_hbm, wq_hbm, wk_hbm, wv_hbm, wo_hbm, wg_hbm, wu_hbm, wd_hbm, out_ref,
    a_rows, knew, vnew, vt, qbuf, bias, cbias, ob, r1, n1, r2, n2, ox, oin, obuf, sbuf_a, sbuf_b, top_a, top_b, wo, wg, wu, wd, part, far, near, mid, b_rows, act,
    load_sem, csem, xs, xr, as_, ar, fs, fr, bs, br, gs, gr, ps, pr, ts, tr, os_, or_, wsem, ss, rs,
):
    x, y, core = place()
    other = 1 - core
    shard_rows, width = x_ref.shape
    heads = qbuf.shape[0]
    slots = ck_hbm.shape[0]
    cached = 2 * slots
    rows = qbuf.shape[3]
    half_rows = shard_rows // 2
    half = width // 2
    tail = pl.ds(cached, rows)
    lo, hi = pl.ds(0, half), pl.ds(half, half)
    a1, a2 = x + core * (y - x), y + core * (x - y)
    sibling, up, down = device(x, y, other), device(x, y + 1, core), device(x, y - 1, core)

    def on1(d):
        return device(x + d * other, y + d * core, core)

    def on2(d):
        return device(x + d * core, y + d * other, core)

    mine = pl.ds(pl.multiple_of(core * slots, slots), slots)

    def head_cols(j, c):
        return pl.ds(pl.multiple_of((2 * j + c) * HEAD_DIM, HEAD_DIM), HEAD_DIM)

    def kept(j, i):
        return wd.at[mine, pl.ds((RING * (1 - i) + j) * HEAD_DIM, HEAD_DIM)]

    local = [pltpu.make_async_copy(src.at[:, head_cols(j, core)], kept(j, i), csem.at[2 * j + i]) for j in range(RING) for i, src in enumerate((ck_hbm, cv_hbm))]
    cross = [remote(src.at[:, head_cols(j, other)], kept(j, i), xs.at[2 * j + i], xr.at[2 * j + i], sibling) for j in range(RING) for i, src in enumerate((ck_hbm, cv_hbm))]
    weights = [pltpu.make_async_copy(src, dst, wsem.at[i]) for i, (src, dst) in enumerate(((wo_hbm, wo), (wg_hbm, wg), (wu_hbm, wu)))]

    def order(i, xg):
        c_part, rest = i // (rows // 2), lax.rem(i, rows // 2)
        t_part, r = rest // shard_rows, lax.rem(rest, shard_rows)
        owner = (2 * xg + c_part) * RING + t_part
        run = jnp.where(r < half_rows, owner, 4 * RING * RING - 1 - owner)
        return run * half_rows + lax.rem(r, half_rows)

    def masks():
        length = len_ref[0]
        for piece in range(2):
            base = ((2 * x + piece) * RING + y) * slots
            slot = base + lax.broadcasted_iota(jnp.int32, (slots, HEAD_DIM), 0)
            lane = lax.broadcasted_iota(jnp.int32, (slots, HEAD_DIM), 1)
            bias[pl.ds(piece * slots, slots)] = jnp.where(jnp.logical_and(slot >= length, lane == 0), HIDDEN, 0.0).astype(jnp.bfloat16)
        key_order = order(lax.broadcasted_iota(jnp.int32, (rows, rows), 0), x)
        for xg in range(RING):
            query_order = order(lax.broadcasted_iota(jnp.int32, (rows, rows), 1), xg)
            cbias[xg] = jnp.where(key_order <= query_order, 0.0, HIDDEN)

    two_lo, two_hi = pl.ds(0, 2), pl.ds(2, 2)

    def q1(g):
        ref = qbuf.at[g, a2, a1]
        return [remote(ref, ref, gs.at[g, i], gr.at[g, i], on1(d)) for i, d in enumerate((2, 1, -1))]

    def q2(g, i):
        d, index, piece, to = ((0, 0, two_lo, 1), (1, 0, two_hi, -1), (2, 0, two_hi, 1), (3, 0, two_lo, -1), (4, -1, two_lo, 1), (5, 1, two_hi, -1))[i]
        ref = qbuf.at[g, ring(a2 + index), piece]
        return remote(ref, ref, gs.at[g, 3 + i], gr.at[g, 3 + i], on2(to))

    def q1_done(g):
        for c in q1(g):
            c.wait_recv()
        for i in range(4):
            q2(g, i).start()

    def q2_relay(g):
        for i in range(2):
            q2(g, i).wait_recv()
            q2(g, 4 + i).start()

    def q2_early(g):
        q2(g, 3).wait_recv()

    def q2_late(g):
        for i in (2, 4, 5):
            q2(g, i).wait_recv()

    pending = []

    def go(c):
        c.start()
        pending.append(c)
        return c

    block = 512

    def turn(j):
        for b in range(cached // block):
            vt[j, :, pl.ds(b * block, block)] = wd[pl.ds(b * block, block), pl.ds(j * HEAD_DIM, HEAD_DIM)].T

    def gather(block, sends, recvs, seen):
        hops = ((0, lo, up), (0, hi, down), (0, hi, up), (0, lo, down), (-1, lo, up), (1, hi, down))
        arrivals = ((-1, lo), (1, hi), (-1, hi), (1, lo), (-2, lo), (2, hi))

        def hop(n):
            d, cols, to = hops[n]
            return remote(block(y + d, cols), block(y + d, cols), sends.at[n], recvs.at[n], to)

        for n in range(4):
            go(hop(n))
        for n, (d, cols) in enumerate(arrivals):
            hop(n).wait_recv()
            if n < 2:
                go(hop(4 + n))
            seen(n, block(y + d, cols), cols)

    loads = []
    wide = heads * HEAD_DIM
    for i, (src, w, at) in enumerate(((wq_hbm, wide, 0), (wk_hbm, HEAD_DIM, wide), (wv_hbm, HEAD_DIM, wide + HEAD_DIM))):
        loads.append(pltpu.make_async_copy(src.at[:, pl.ds(pl.multiple_of(core * w, w), w)], wg.at[:, pl.ds(at, w)], load_sem.at[i]))
        loads[-1].start()
    for c in local:
        c.start()
    partners = (sibling, *(on(d) for on in (on1, on2) for d in (1, -1, 2)))
    greet(partners)
    a_rows[core, y] = normalize(x_ref[...].astype(jnp.float32), gain1_ref[...].reshape(1, width))
    pl.semaphore_wait(pltpu.get_barrier_semaphore(), len(partners))
    whole = pl.ds(0, width)

    def row_block(c):
        return lambda i, cols: a_rows.at[c, ring(i), :, cols]

    def forward(n, block, cols):
        go(remote(block, block, fs.at[n], fr.at[n], sibling))
        if n == 1:
            for c in cross:
                c.start()

    own = row_block(core)(y, whole)
    go(remote(own, own, fs.at[6], fr.at[6], sibling))
    gather(row_block(core), as_, ar, forward)
    for n, (d, cols) in enumerate(((-1, lo), (1, hi), (-1, hi), (1, lo), (-2, lo), (2, hi), (0, whole))):
        ref = row_block(other)(y + d, cols)
        remote(ref, ref, fs.at[n], fr.at[n], sibling).wait_recv()
    for load in loads:
        load.wait()
    a = a_rows[...].reshape(rows, width)
    cos, sin = cos_ref[...], sin_ref[...]

    def rotate(p):
        return (p * cos + pltpu.roll(p, HEAD_DIM // 2, axis=1) * sin).astype(jnp.bfloat16)

    q = dot(a, wg[:, :wide])
    for g in range(heads):
        qbuf[g, a2, a1] = rotate(q[:, g * HEAD_DIM : (g + 1) * HEAD_DIM])
        for c in q1(g):
            c.start()
    knew[...] = rotate(dot(a, wg[:, wide : wide + HEAD_DIM]))
    vnew[...] = dot(a, wg[:, wide + HEAD_DIM : wide + 2 * HEAD_DIM]).T.astype(jnp.bfloat16)
    masks()
    for i in range(2 * RING):
        local[i].wait()
        cross[i].wait_recv()
    turn(0)
    for g in range(heads):
        q1_done(g)
    for j in range(1, RING):
        turn(j)

    def back(g, h):
        flip = (g + 1) // heads
        return h + flip - 2 * flip * h

    def granule(g, h):
        return ring(a2 - back(g, h)), ring(a2 + 1 + back(g, h))

    def first(g, h, straight=False):
        far, near_up, near_down = ring(a1 + 2), ring(a1 + 1), ring(a1 - 1)
        even, odd = granule(g, h)

        def hop(i, src, dst, target):
            return remote(src, dst, ps.at[g, h, i], pr.at[g, h, i], target)

        return (
            lambda: hop(0, ob.at[g, far, even], r1.at[g, h, 0], on1(2 if straight else 1)),
            lambda: hop(1, ob.at[g, far, odd], r1.at[g, h, 1], on1(2 if straight else -1)),
            lambda: hop(2, ob.at[g, near_up, odd], n1.at[g, 0, odd], on1(1)),
            lambda: hop(3, ob.at[g, near_down, even], n1.at[g, 1, even], on1(-1)),
            lambda: hop(4, ob.at[g, near_up, even], n1.at[g, 0, even], on1(1)),
            lambda: hop(5, ob.at[g, near_down, odd], n1.at[g, 1, odd], on1(-1)),
        )

    def second(g):
        def hop(i, d, dst):
            return lambda: remote(ob.at[g, a1, ring(a2 + d)], dst, ts.at[g, i], tr.at[g, i], on2(d))

        return hop(0, 2, r2.at[g]), hop(1, -1, n2.at[g, 0]), hop(2, 1, n2.at[g, 1])

    def swap(g):
        give = pl.ds(pl.multiple_of(other * (rows // 2), rows // 2), rows // 2)
        return remote(ox.at[g, give], oin.at[g], os_.at[g], or_.at[g], sibling)

    def reduce_0(g, h, straight):
        copies = first(g, h, straight)
        for c in copies if straight else copies[:4]:
            c().start()

    def reduce_1(g, h):
        copies = first(g, h)
        for i, b in enumerate(granule(g, h)):
            copies[i]().wait_recv()
            to = ring(a1 + 1 - 2 * i)
            put_block(ob, (g, to, b), *merge([ob[g, to, b], r1[g, h, i]]))
            copies[4 + i]().start()

    def reduce_2(g, h, straight=False):
        for c in first(g, h)[0 if straight else 2 :]:
            c().wait_recv()
        for i, b in enumerate(granule(g, h)):
            put_block(ob, (g, a1, b), *merge([ob[g, a1, b], n1[g, 0, b], n1[g, 1, b]] + ([r1[g, h, i]] if straight else [])))

        @pl.when(back(g, h) == 0)
        def _():
            second(g)[2]().start()

        @pl.when(back(g, h) == 1)
        def _():
            second(g)[0]().start()
            second(g)[1]().start()

    def reduce_3(g):
        for c in second(g):
            c().wait_recv()
        total, _, norm = merge([ob[g, a1, a2], n2[g, 0], n2[g, 1], r2[g]])
        ox[g] = (total / norm).T.astype(jnp.bfloat16)
        swap(g).start()

    def unit(u):
        g, h, i = u // 8, lax.rem(u // 4, 2), lax.rem(u, 4)
        near, far_off = granule(g, h)
        t = (near + (i // 2) * (far_off - near)) * other + i * core
        pair = [(2 * lax.rem(i, 2) + n) * other + (near, far_off)[n] * core for n in range(2)]
        places = [(g, xg + core * (t - xg), t + core * (xg - t)) for xg in pair]
        return t, pair, places

    step = 512
    chunks = [pl.ds(b * step, step) for b in range(cached // step)] + [tail]

    def keys_at(t):
        return pl.ds(pl.multiple_of((RING + t) * HEAD_DIM, HEAD_DIM), HEAD_DIM)

    def advance(ahead, s_out, top_out, u, s_in, top_in):
        if ahead is not None:
            t_next, pair, q_places = unit(ahead)
            q = jnp.concatenate([qbuf[g, p2, p1] for g, p1, p2 in q_places], axis=0)
            unit_col = jnp.where(lax.broadcasted_iota(jnp.int32, q.shape, 1) == 0, 1.0, 0.0).astype(jnp.bfloat16)
            deep_q = jnp.concatenate([q, unit_col], axis=1)
            unseen = jnp.where(t_next == y, 0.0, HIDDEN)
            peak = jnp.full((8, 2 * rows), -jnp.inf, jnp.float32)
        if u is not None:
            t, _, places = unit(u)
            top = top_in[...]
            norm, total = jnp.zeros((8, 2 * rows), jnp.float32), 0.0
        for at in chunks:
            if ahead is not None:
                if at is tail:
                    s = dot_nt(knew[...], q) + (jnp.concatenate([cbias[xg] for xg in pair], axis=1) + unseen)
                else:
                    s = dot_nt(jnp.concatenate([wd[at, keys_at(t_next)], bias[at]], axis=1), deep_q)
                s_out[at] = s
                peak = jnp.maximum(peak, jnp.max(s.reshape(-1, 8, 2 * rows), axis=0))
            if u is not None:
                e = jnp.exp2(s_in[at] * SCALE2 - top)
                norm = norm + jnp.sum(e.reshape(-1, 8, 2 * rows), axis=0)
                total = total + dot(vnew[...] if at is tail else vt[t, :, at], e.astype(jnp.bfloat16))
        if ahead is not None:
            top_out[...] = jnp.max(peak, axis=0, keepdims=True) * SCALE2
        if u is not None:
            norm = jnp.sum(norm, axis=0, keepdims=True)
            for n, index in enumerate(places):
                cut = slice(n * rows, (n + 1) * rows)
                put_block(ob, index, total[:, cut], top[:, cut], norm[:, cut])

    q2_relay(0)
    q2_early(0)
    for w in weights:
        w.start()
    units = heads * 8
    advance(0, sbuf_a, top_a, None, None, None)

    @pl.loop(0, units // 2)
    def _(i):
        @pl.when(i == 1)
        def _():
            q2_late(0)

        for g in range(1, heads):
            @pl.when(i == 4 * g - 1)
            def _():
                q2_early(g)
                q2_late(g)

        u = 2 * i
        advance(u + 1, sbuf_b, top_b, u, sbuf_a, top_a)
        advance(jnp.minimum(u + 2, units - 1), sbuf_a, top_a, u + 1, sbuf_b, top_b)

        for g in range(1, heads):
            @pl.when(i == g - 1)
            def _():
                q2_relay(g)

        n = i // 2
        late = lax.rem(i, 2) == 1

        @pl.when(jnp.logical_and(late, n < 2 * heads - 1))
        def _():
            reduce_0(n // 2, lax.rem(n, 2), False)

        @pl.when(jnp.logical_and(late, n == 2 * heads - 1))
        def _():
            reduce_0(heads - 1, 1, False)

        @pl.when(jnp.logical_and(late, n >= 1))
        def _():
            reduce_1((n - 1) // 2, lax.rem(n - 1, 2))

        @pl.when(jnp.logical_and(late, n >= 3))
        def _():
            reduce_2((n - 3) // 2, lax.rem(n - 3, 2))


    cols = width // RING
    sent = []

    def settle():
        while sent:
            sent.pop().wait_send()

    def reduce_rows(n, product):
        quarter = [pl.ds(i * cols, cols) for i in range(RING)]
        near_up, near_down = ring(y + 1), ring(y - 1)

        def hop(i, src, dst, target):
            return remote(src, dst, ss.at[n, i], rs.at[n, i], target)

        a_hops = [hop(i, part.at[ring(y + 2), :, q], far.at[n, :, q], up if i < 2 else down) for i, q in enumerate(quarter)]
        b_hops = [hop(4, part.at[near_up, :, hi], near.at[n, 0, :, hi], up), hop(5, part.at[near_down, :, lo], near.at[n, 1, :, lo], down)]
        c_hops = [hop(6 + i, part.at[near_up if i < 2 else near_down, :, q], near.at[n, i // 2, :, q], up if i < 2 else down) for i, q in enumerate(quarter)]
        turns = (0, 2, 1, 3)
        for i in turns:
            part[:, :, quarter[i]] = product(quarter[i]).reshape(RING, shard_rows, cols)
            a_hops[i].start()
        for c in b_hops:
            c.start()
        for i in turns:
            a_hops[i].wait_recv()
            to = near_up if i < 2 else near_down
            part[to, :, quarter[i]] = part[to, :, quarter[i]] + far[n, :, quarter[i]]
            c_hops[i].start()
        for c in b_hops + c_hops:
            c.wait_recv()
        sent.extend(a_hops + b_hops + c_hops)
        return part[y] + (near[n, 0] + near[n, 1])

    down_load = pltpu.make_async_copy(wd_hbm, wd, wsem.at[3])
    down_load.start()
    last = heads - 1
    reduce_2(last - 1, 1)
    reduce_1(last, 1)
    reduce_2(last, 0)
    reduce_3(0)
    for g in range(1, last):
        reduce_3(g)
    reduce_2(last, 1)
    reduce_3(last)
    keep = pl.ds(pl.multiple_of(core * (rows // 2), rows // 2), rows // 2)
    obuf[core] = ox[:, keep]
    for g in range(heads):
        swap(g).wait_recv()
    obuf[other] = oin[...]
    o = jnp.concatenate([obuf[c, g] for c in range(2) for g in range(heads)], axis=1)
    weights[0].wait()
    h = (x_ref[...].astype(jnp.float32) + reduce_rows(0, lambda at: dot(o, wo[:, at]))).astype(jnp.bfloat16)
    mid[...] = h
    b_rows[y] = normalize(h.astype(jnp.float32), gain2_ref[...].reshape(1, width))

    gather(lambda i, cut: b_rows.at[ring(i), :, cut], bs, br, lambda *_: None)
    b = b_rows[...].reshape(RING * shard_rows, width)
    weights[1].wait()
    weights[2].wait()
    wide = act.shape[1] // 2

    @pl.loop(0, act.shape[1] // wide)
    def _(i):
        at = pl.ds(pl.multiple_of(i * wide, wide), wide)
        gate = dot(b, wg[:, at])
        act[:, at] = (gate * jax.nn.sigmoid(gate) * dot(b, wu[:, at])).astype(jnp.bfloat16)

    down_load.wait()
    inner = act[...]

    settle()
    out_ref[...] = (mid[...].astype(jnp.float32) + reduce_rows(1, lambda at: dot(inner, wd[:, at]))).astype(jnp.bfloat16)
    settle()
    for c in pending + cross:
        c.wait_send()
    for g in range(heads):
        for c in q1(g) + [q2(g, i) for i in range(6)]:
            c.wait_send()
        for c in (*first(g, 0), *first(g, 1), *second(g)):
            c().wait_send()
        swap(g).wait_send()


def layer(cache_len, hidden, gain1, gain2, cos, sin, cache_k, cache_v, w_query, w_key, w_value, w_out, w_gate, w_up, w_down):
    shard_rows, width = hidden.shape
    kv_local = w_key.shape[1] // HEAD_DIM
    heads = w_query.shape[1] // w_key.shape[1]
    rows = 2 * RING * shard_rows
    slots = cache_k.shape[0]
    total = 2 * slots + rows
    inner = w_gate.shape[1]
    deep = HEAD_DIM + 8
    assert kv_local == 2 and w_down.shape[0] >= 2 * slots and width >= 2 * RING * HEAD_DIM and inner >= (heads + 2) * HEAD_DIM and cache_k.shape[1] == 2 * RING * HEAD_DIM
    bf16, f32 = jnp.bfloat16, jnp.float32
    vmem, hbm, smem = pl.BlockSpec(memory_space=pltpu.VMEM), pl.BlockSpec(memory_space=pl.ANY), pl.BlockSpec(memory_space=pltpu.SMEM)
    dma = pltpu.SemaphoreType.DMA
    return pl.pallas_call(
        layer_kernel,
        out_shape=jax.ShapeDtypeStruct(hidden.shape, bf16),
        in_specs=[smem] + [vmem] * 5 + [hbm] * 9,
        out_specs=vmem,
        scratch_shapes=[
            pltpu.VMEM((2, RING, shard_rows, width), bf16),
            pltpu.VMEM((rows, HEAD_DIM), bf16),
            pltpu.VMEM((HEAD_DIM, rows), bf16),
            pltpu.VMEM((RING, HEAD_DIM, 2 * slots), bf16),
            pltpu.VMEM((heads, RING, RING, rows, HEAD_DIM), bf16),
            pltpu.VMEM((2 * slots, HEAD_DIM), bf16),
            pltpu.VMEM((RING, rows, rows), f32),
            pltpu.VMEM((heads, RING, RING, deep, rows), f32),
            pltpu.VMEM((heads, 2, 2, deep, rows), f32),
            pltpu.VMEM((heads, 2, RING, deep, rows), f32),
            pltpu.VMEM((heads, deep, rows), f32),
            pltpu.VMEM((heads, 2, deep, rows), f32),
            pltpu.VMEM((heads, rows, HEAD_DIM), bf16),
            pltpu.VMEM((heads, rows // 2, HEAD_DIM), bf16),
            pltpu.VMEM((2, heads, rows // 2, HEAD_DIM), bf16),
            pltpu.VMEM((total, 2 * rows), f32),
            pltpu.VMEM((total, 2 * rows), f32),
            pltpu.VMEM((1, 2 * rows), f32),
            pltpu.VMEM((1, 2 * rows), f32),
            pltpu.VMEM(w_out.shape, bf16),
            pltpu.VMEM(w_gate.shape, bf16),
            pltpu.VMEM(w_up.shape, bf16),
            pltpu.VMEM(w_down.shape, bf16),
            pltpu.VMEM((RING, shard_rows, width), f32),
            pltpu.VMEM((2, shard_rows, width), f32),
            pltpu.VMEM((2, 2, shard_rows, width), f32),
            pltpu.VMEM((shard_rows, width), bf16),
            pltpu.VMEM((RING, shard_rows, width), bf16),
            pltpu.VMEM((RING * shard_rows, inner), bf16),
            dma((3,)),
            dma((2 * RING,)),
            *(dma(shape) for shape in ((2 * RING,), (6,), (7,), (6,), (heads, 9), (heads, 2, 6), (heads, 3), (heads,)) for _ in range(2)),
            dma((4,)),
            dma((2, 10)),
            dma((2, 10)),
        ],
        compiler_params=pltpu.CompilerParams(collective_id=0, has_side_effects=True, vmem_limit_bytes=VMEM_LIMIT),
        name='attend',
    )(cache_len, hidden, gain1, gain2, cos, sin, cache_k, cache_v, w_query, w_key, w_value, w_out, w_gate, w_up, w_down)


def solution(mesh):
    devices = mesh.shape['tp'] * mesh.shape['cp']
    assert mesh.shape['tp'] == RING and mesh.shape['cp'] == 2 * RING
    token_spec = P(('dp', 'cp', 'tp'), None)
    column_spec = P(None, 'tp')
    row_spec = P('tp', None)

    def tables(cache_len, shard_rows):
        half_rows, half_dim = shard_rows // 2, HEAD_DIM // 2
        row = jnp.arange(2 * RING * shard_rows, dtype=jnp.int32)
        owner = (lax.axis_index('cp') // 2) * (2 * RING) + row // shard_rows
        r = row % shard_rows
        run = jnp.where(r < half_rows, owner, 2 * devices - 1 - owner)
        pos = cache_len[0] + run * half_rows + r % half_rows
        inv_freq = 1.0 / (ROPE_BASE ** (jnp.arange(half_dim, dtype=jnp.float32) * (2.0 / HEAD_DIM)))
        angles = pos.astype(jnp.float32)[:, None] * inv_freq[None, :]
        cos, sin = jnp.cos(angles), jnp.sin(angles)
        return jnp.concatenate([cos, cos], axis=1), jnp.concatenate([-sin, sin], axis=1)

    def device_layer(hidden, pos, cache_len, cache_k, cache_v, norm1_gain, w_query, w_key, w_value, w_out, norm2_gain, w_gate, w_up, w_down):
        cos, sin = tables(cache_len, hidden.shape[0])
        return layer(cache_len, hidden, norm1_gain, norm2_gain, cos, sin, cache_k, cache_v, w_query, w_key, w_value, w_out, w_gate, w_up, w_down)

    return jax.shard_map(device_layer, mesh=mesh, in_specs=(token_spec, P(('dp', 'cp', 'tp')), P('dp'), token_spec, token_spec, P(), column_spec, column_spec, column_spec, row_spec, P(), column_spec, column_spec, row_spec), out_specs=token_spec, check_vma=False)
```

```python
import functools
import math

import jax
import jax.numpy as jnp
from jax import lax
from jax.experimental import pallas as pl
from jax.experimental.pallas import tpu as pltpu
from jax.sharding import PartitionSpec as P

HEAD_DIM = 128
ROPE_BASE = 500000.0
NORM_EPS = 1e-5
HIDDEN = -1e38
SCALE2 = math.log2(math.e) / math.sqrt(HEAD_DIM)
MESH = pl.DeviceIdType.MESH
RING = 4
VMEM_LIMIT = 67_043_328


def place():
    c = lax.axis_index('cp')
    return c // 2, lax.axis_index('tp'), lax.rem(c, 2)


def ring(i):
    return lax.rem(i + RING, RING)


def device(x, y, core):
    return {'tp': ring(y), 'cp': 2 * ring(x) + core}


def remote(src, dst, send_sem, recv_sem, target):
    return pltpu.make_async_remote_copy(src_ref=src, dst_ref=dst, send_sem=send_sem, recv_sem=recv_sem, device_id=target, device_id_type=MESH)


def greet(partners):
    for partner in partners:
        pl.semaphore_signal(pltpu.get_barrier_semaphore(), inc=1, device_id=partner, device_id_type=MESH)


def normalize(values, gain):
    inv_rms = lax.rsqrt(jnp.mean(values * values, axis=-1, keepdims=True) + NORM_EPS)
    return (values * inv_rms * gain.astype(jnp.float32)).astype(jnp.bfloat16)


def dot(a, b):
    return jnp.dot(a, b, preferred_element_type=jnp.float32)


def dot_nt(a, b):
    return lax.dot_general(a, b, (((1,), (1,)), ((), ())), preferred_element_type=jnp.float32)


def merge(parts):
    top = parts[0][HEAD_DIM : HEAD_DIM + 1]
    for p in parts[1:]:
        top = jnp.maximum(top, p[HEAD_DIM : HEAD_DIM + 1])
    total, norm = 0.0, 0.0
    for p in parts:
        weight = jnp.exp2(p[HEAD_DIM : HEAD_DIM + 1] - top)
        total = total + p[:HEAD_DIM] * weight
        norm = norm + p[HEAD_DIM + 1 : HEAD_DIM + 2] * weight
    return total, top, norm


def put_block(ref, index, total, top, norm):
    ref[(*index, pl.ds(0, HEAD_DIM))] = total
    ref[(*index, pl.ds(HEAD_DIM, 8))] = jnp.concatenate([top, norm, jnp.zeros((6, total.shape[1]), jnp.float32)], axis=0)


def layer_kernel(
    len_ref, x_ref, gain1_ref, gain2_ref, cos_ref, sin_ref, ck_hbm, cv_hbm, wq_hbm, wk_hbm, wv_hbm, wo_hbm, wg_hbm, wu_hbm, wd_hbm, out_ref,
    a_rows, knew, vnew, vt, qbuf, bias, cbias, ob, r1, n1, r2, n2, ox, oin, obuf, sbuf_a, sbuf_b, top_a, top_b, wo, wg, wu, wd, part, far, near, mid, b_rows, act,
    load_sem, csem, xs, xr, as_, ar, fs, fr, bs, br, gs, gr, ps, pr, ts, tr, os_, or_, wsem, ss, rs,
):
    x, y, core = place()
    other = 1 - core
    shard_rows, width = x_ref.shape
    heads = qbuf.shape[0]
    slots = ck_hbm.shape[0]
    cached = 2 * slots
    rows = qbuf.shape[3]
    half_rows = shard_rows // 2
    half = width // 2
    tail = pl.ds(cached, rows)
    lo, hi = pl.ds(0, half), pl.ds(half, half)
    a1, a2 = x + core * (y - x), y + core * (x - y)
    sibling, up, down = device(x, y, other), device(x, y + 1, core), device(x, y - 1, core)

    def on1(d):
        return device(x + d * other, y + d * core, core)

    def on2(d):
        return device(x + d * core, y + d * other, core)

    mine = pl.ds(pl.multiple_of(core * slots, slots), slots)

    def head_cols(j, c):
        return pl.ds(pl.multiple_of((2 * j + c) * HEAD_DIM, HEAD_DIM), HEAD_DIM)

    def kept(j, i):
        return wd.at[mine, pl.ds((RING * (1 - i) + j) * HEAD_DIM, HEAD_DIM)]

    local = [pltpu.make_async_copy(src.at[:, head_cols(j, core)], kept(j, i), csem.at[2 * j + i]) for j in range(RING) for i, src in enumerate((ck_hbm, cv_hbm))]
    cross = [remote(src.at[:, head_cols(j, other)], kept(j, i), xs.at[2 * j + i], xr.at[2 * j + i], sibling) for j in range(RING) for i, src in enumerate((ck_hbm, cv_hbm))]
    weights = [pltpu.make_async_copy(src, dst, wsem.at[i]) for i, (src, dst) in enumerate(((wo_hbm, wo), (wg_hbm, wg), (wu_hbm, wu)))]

    def order(i, xg):
        c_part, rest = i // (rows // 2), lax.rem(i, rows // 2)
        t_part, r = rest // shard_rows, lax.rem(rest, shard_rows)
        owner = (2 * xg + c_part) * RING + t_part
        run = jnp.where(r < half_rows, owner, 4 * RING * RING - 1 - owner)
        return run * half_rows + lax.rem(r, half_rows)

    def masks():
        length = len_ref[0]
        for piece in range(2):
            base = ((2 * x + piece) * RING + y) * slots
            slot = base + lax.broadcasted_iota(jnp.int32, (slots, HEAD_DIM), 0)
            lane = lax.broadcasted_iota(jnp.int32, (slots, HEAD_DIM), 1)
            bias[pl.ds(piece * slots, slots)] = jnp.where(jnp.logical_and(slot >= length, lane == 0), HIDDEN, 0.0).astype(jnp.bfloat16)
        key_order = order(lax.broadcasted_iota(jnp.int32, (rows, rows), 0), x)
        for xg in range(RING):
            query_order = order(lax.broadcasted_iota(jnp.int32, (rows, rows), 1), xg)
            cbias[xg] = jnp.where(key_order <= query_order, 0.0, HIDDEN)

    two_lo, two_hi = pl.ds(0, 2), pl.ds(2, 2)

    def q1(g):
        ref = qbuf.at[g, a2, a1]
        return [remote(ref, ref, gs.at[g, i], gr.at[g, i], on1(d)) for i, d in enumerate((2, 1, -1))]

    def q2(g, i):
        d, index, piece, to = ((0, 0, two_lo, 1), (1, 0, two_hi, -1), (2, 0, two_hi, 1), (3, 0, two_lo, -1), (4, -1, two_lo, 1), (5, 1, two_hi, -1))[i]
        ref = qbuf.at[g, ring(a2 + index), piece]
        return remote(ref, ref, gs.at[g, 3 + i], gr.at[g, 3 + i], on2(to))

    def q1_done(g):
        for c in q1(g):
            c.wait_recv()
        for i in range(4):
            q2(g, i).start()

    def q2_relay(g):
        for i in range(2):
            q2(g, i).wait_recv()
            q2(g, 4 + i).start()

    def q2_early(g):
        q2(g, 3).wait_recv()

    def q2_late(g):
        for i in (2, 4, 5):
            q2(g, i).wait_recv()

    pending = []

    def go(c):
        c.start()
        pending.append(c)
        return c

    block = 512

    def turn(j):
        for b in range(cached // block):
            vt[j, :, pl.ds(b * block, block)] = wd[pl.ds(b * block, block), pl.ds(j * HEAD_DIM, HEAD_DIM)].T

    def gather(block, sends, recvs, seen):
        hops = ((0, lo, up), (0, hi, down), (0, hi, up), (0, lo, down), (-1, lo, up), (1, hi, down))
        arrivals = ((-1, lo), (1, hi), (-1, hi), (1, lo), (-2, lo), (2, hi))

        def hop(n):
            d, cols, to = hops[n]
            return remote(block(y + d, cols), block(y + d, cols), sends.at[n], recvs.at[n], to)

        for n in range(4):
            go(hop(n))
        for n, (d, cols) in enumerate(arrivals):
            hop(n).wait_recv()
            if n < 2:
                go(hop(4 + n))
            seen(n, block(y + d, cols), cols)

    loads = []
    wide = heads * HEAD_DIM
    for i, (src, w, at) in enumerate(((wq_hbm, wide, 0), (wk_hbm, HEAD_DIM, wide), (wv_hbm, HEAD_DIM, wide + HEAD_DIM))):
        loads.append(pltpu.make_async_copy(src.at[:, pl.ds(pl.multiple_of(core * w, w), w)], wg.at[:, pl.ds(at, w)], load_sem.at[i]))
        loads[-1].start()
    for c in local:
        c.start()
    partners = (sibling, *(on(d) for on in (on1, on2) for d in (1, -1, 2)))
    greet(partners)
    a_rows[core, y] = normalize(x_ref[...].astype(jnp.float32), gain1_ref[...].reshape(1, width))
    pl.semaphore_wait(pltpu.get_barrier_semaphore(), len(partners))
    whole = pl.ds(0, width)

    def row_block(c):
        return lambda i, cols: a_rows.at[c, ring(i), :, cols]

    def forward(n, block, cols):
        go(remote(block, block, fs.at[n], fr.at[n], sibling))
        if n == 1:
            for c in cross:
                c.start()

    own = row_block(core)(y, whole)
    go(remote(own, own, fs.at[6], fr.at[6], sibling))
    gather(row_block(core), as_, ar, forward)
    for n, (d, cols) in enumerate(((-1, lo), (1, hi), (-1, hi), (1, lo), (-2, lo), (2, hi), (0, whole))):
        ref = row_block(other)(y + d, cols)
        remote(ref, ref, fs.at[n], fr.at[n], sibling).wait_recv()
    for load in loads:
        load.wait()
    a = a_rows[...].reshape(rows, width)
    cos, sin = cos_ref[...], sin_ref[...]

    def rotate(p):
        return (p * cos + pltpu.roll(p, HEAD_DIM // 2, axis=1) * sin).astype(jnp.bfloat16)

    q = dot(a, wg[:, :wide])
    for g in range(heads):
        qbuf[g, a2, a1] = rotate(q[:, g * HEAD_DIM : (g + 1) * HEAD_DIM])
        for c in q1(g):
            c.start()
    knew[...] = rotate(dot(a, wg[:, wide : wide + HEAD_DIM]))
    vnew[...] = dot(a, wg[:, wide + HEAD_DIM : wide + 2 * HEAD_DIM]).T.astype(jnp.bfloat16)
    masks()
    for i in range(2 * RING):
        local[i].wait()
        cross[i].wait_recv()
    turn(0)
    for g in range(heads):
        q1_done(g)
    for j in range(1, RING):
        turn(j)

    def back(g, h):
        flip = (g + 1) // heads
        return h + flip - 2 * flip * h

    def granule(g, h):
        return ring(a2 - back(g, h)), ring(a2 + 1 + back(g, h))

    def first(g, h, straight=False):
        far, near_up, near_down = ring(a1 + 2), ring(a1 + 1), ring(a1 - 1)
        even, odd = granule(g, h)

        def hop(i, src, dst, target):
            return remote(src, dst, ps.at[g, h, i], pr.at[g, h, i], target)

        return (
            lambda: hop(0, ob.at[g, far, even], r1.at[g, h, 0], on1(2 if straight else 1)),
            lambda: hop(1, ob.at[g, far, odd], r1.at[g, h, 1], on1(2 if straight else -1)),
            lambda: hop(2, ob.at[g, near_up, odd], n1.at[g, 0, odd], on1(1)),
            lambda: hop(3, ob.at[g, near_down, even], n1.at[g, 1, even], on1(-1)),
            lambda: hop(4, ob.at[g, near_up, even], n1.at[g, 0, even], on1(1)),
            lambda: hop(5, ob.at[g, near_down, odd], n1.at[g, 1, odd], on1(-1)),
        )

    def second(g):
        def hop(i, d, dst):
            return lambda: remote(ob.at[g, a1, ring(a2 + d)], dst, ts.at[g, i], tr.at[g, i], on2(d))

        return hop(0, 2, r2.at[g]), hop(1, -1, n2.at[g, 0]), hop(2, 1, n2.at[g, 1])

    def swap(g):
        give = pl.ds(pl.multiple_of(other * (rows // 2), rows // 2), rows // 2)
        return remote(ox.at[g, give], oin.at[g], os_.at[g], or_.at[g], sibling)

    def reduce_0(g, h, straight):
        copies = first(g, h, straight)
        for c in copies if straight else copies[:4]:
            c().start()

    def reduce_1(g, h):
        copies = first(g, h)
        for i, b in enumerate(granule(g, h)):
            copies[i]().wait_recv()
            to = ring(a1 + 1 - 2 * i)
            put_block(ob, (g, to, b), *merge([ob[g, to, b], r1[g, h, i]]))
            copies[4 + i]().start()

    def reduce_2(g, h, straight=False):
        for c in first(g, h)[0 if straight else 2 :]:
            c().wait_recv()
        for i, b in enumerate(granule(g, h)):
            put_block(ob, (g, a1, b), *merge([ob[g, a1, b], n1[g, 0, b], n1[g, 1, b]] + ([r1[g, h, i]] if straight else [])))

        @pl.when(back(g, h) == 0)
        def _():
            second(g)[2]().start()

        @pl.when(back(g, h) == 1)
        def _():
            second(g)[0]().start()
            second(g)[1]().start()

    def reduce_3(g):
        for c in second(g):
            c().wait_recv()
        total, _, norm = merge([ob[g, a1, a2], n2[g, 0], n2[g, 1], r2[g]])
        ox[g] = (total / norm).T.astype(jnp.bfloat16)
        swap(g).start()

    def unit(u):
        g, h, i = u // 8, lax.rem(u // 4, 2), lax.rem(u, 4)
        near, far_off = granule(g, h)
        t = (near + (i // 2) * (far_off - near)) * other + i * core
        pair = [(2 * lax.rem(i, 2) + n) * other + (near, far_off)[n] * core for n in range(2)]
        places = [(g, xg + core * (t - xg), t + core * (xg - t)) for xg in pair]
        return t, pair, places

    step = 512
    chunks = [pl.ds(b * step, step) for b in range(cached // step)] + [tail]

    def keys_at(t):
        return pl.ds(pl.multiple_of((RING + t) * HEAD_DIM, HEAD_DIM), HEAD_DIM)

    def advance(ahead, s_out, top_out, u, s_in, top_in):
        if ahead is not None:
            t_next, pair, q_places = unit(ahead)
            q = jnp.concatenate([qbuf[g, p2, p1] for g, p1, p2 in q_places], axis=0)
            unit_col = jnp.where(lax.broadcasted_iota(jnp.int32, q.shape, 1) == 0, 1.0, 0.0).astype(jnp.bfloat16)
            deep_q = jnp.concatenate([q, unit_col], axis=1)
            unseen = jnp.where(t_next == y, 0.0, HIDDEN)
            peak = jnp.full((8, 2 * rows), -jnp.inf, jnp.float32)
        if u is not None:
            t, _, places = unit(u)
            top = top_in[...]
            norm, total = jnp.zeros((8, 2 * rows), jnp.float32), 0.0
        for at in chunks:
            if ahead is not None:
                if at is tail:
                    s = dot_nt(knew[...], q) + (jnp.concatenate([cbias[xg] for xg in pair], axis=1) + unseen)
                else:
                    s = dot_nt(jnp.concatenate([wd[at, keys_at(t_next)], bias[at]], axis=1), deep_q)
                s_out[at] = s
                peak = jnp.maximum(peak, jnp.max(s.reshape(-1, 8, 2 * rows), axis=0))
            if u is not None:
                e = jnp.exp2(s_in[at] * SCALE2 - top)
                norm = norm + jnp.sum(e.reshape(-1, 8, 2 * rows), axis=0)
                total = total + dot(vnew[...] if at is tail else vt[t, :, at], e.astype(jnp.bfloat16))
        if ahead is not None:
            top_out[...] = jnp.max(peak, axis=0, keepdims=True) * SCALE2
        if u is not None:
            norm = jnp.sum(norm, axis=0, keepdims=True)
            for n, index in enumerate(places):
                cut = slice(n * rows, (n + 1) * rows)
                put_block(ob, index, total[:, cut], top[:, cut], norm[:, cut])

    q2_relay(0)
    q2_early(0)
    for w in weights:
        w.start()
    units = heads * 8
    advance(0, sbuf_a, top_a, None, None, None)

    @pl.loop(0, units // 2)
    def _(i):
        @pl.when(i == 1)
        def _():
            q2_late(0)

        for g in range(1, heads):
            @pl.when(i == 4 * g - 1)
            def _():
                q2_early(g)
                q2_late(g)

        u = 2 * i
        advance(u + 1, sbuf_b, top_b, u, sbuf_a, top_a)
        advance(jnp.minimum(u + 2, units - 1), sbuf_a, top_a, u + 1, sbuf_b, top_b)

        for g in range(1, heads):
            @pl.when(i == g - 1)
            def _():
                q2_relay(g)

        n = i // 2
        late = lax.rem(i, 2) == 1

        @pl.when(jnp.logical_and(late, n < 2 * heads - 1))
        def _():
            reduce_0(n // 2, lax.rem(n, 2), False)

        @pl.when(jnp.logical_and(late, n == 2 * heads - 1))
        def _():
            reduce_0(heads - 1, 1, False)

        @pl.when(jnp.logical_and(late, n >= 1))
        def _():
            reduce_1((n - 1) // 2, lax.rem(n - 1, 2))

        @pl.when(jnp.logical_and(late, n >= 3))
        def _():
            reduce_2((n - 3) // 2, lax.rem(n - 3, 2))


    cols = width // RING
    sent = []

    def settle():
        while sent:
            sent.pop().wait_send()

    def reduce_rows(n, product):
        quarter = [pl.ds(i * cols, cols) for i in range(RING)]
        near_up, near_down = ring(y + 1), ring(y - 1)

        def hop(i, src, dst, target):
            return remote(src, dst, ss.at[n, i], rs.at[n, i], target)

        a_hops = [hop(i, part.at[ring(y + 2), :, q], far.at[n, :, q], up if i < 2 else down) for i, q in enumerate(quarter)]
        b_hops = [hop(4, part.at[near_up, :, hi], near.at[n, 0, :, hi], up), hop(5, part.at[near_down, :, lo], near.at[n, 1, :, lo], down)]
        c_hops = [hop(6 + i, part.at[near_up if i < 2 else near_down, :, q], near.at[n, i // 2, :, q], up if i < 2 else down) for i, q in enumerate(quarter)]
        turns = (0, 2, 1, 3)
        for i in turns:
            part[:, :, quarter[i]] = product(quarter[i]).reshape(RING, shard_rows, cols)
            a_hops[i].start()
        for c in b_hops:
            c.start()
        for i in turns:
            a_hops[i].wait_recv()
            to = near_up if i < 2 else near_down
            part[to, :, quarter[i]] = part[to, :, quarter[i]] + far[n, :, quarter[i]]
            c_hops[i].start()
        for c in b_hops + c_hops:
            c.wait_recv()
        sent.extend(a_hops + b_hops + c_hops)
        return part[y] + (near[n, 0] + near[n, 1])

    down_load = pltpu.make_async_copy(wd_hbm, wd, wsem.at[3])
    down_load.start()
    last = heads - 1
    reduce_2(last - 1, 1)
    reduce_1(last, 1)
    reduce_2(last, 0)
    reduce_2(last, 1)
    for g in range(last):
        reduce_3(g)
    reduce_3(last)
    keep = pl.ds(pl.multiple_of(core * (rows // 2), rows // 2), rows // 2)
    obuf[core] = ox[:, keep]
    for g in range(heads):
        swap(g).wait_recv()
    obuf[other] = oin[...]
    o = jnp.concatenate([obuf[c, g] for c in range(2) for g in range(heads)], axis=1)
    weights[0].wait()
    h = (x_ref[...].astype(jnp.float32) + reduce_rows(0, lambda at: dot(o, wo[:, at]))).astype(jnp.bfloat16)
    mid[...] = h
    b_rows[y] = normalize(h.astype(jnp.float32), gain2_ref[...].reshape(1, width))

    gather(lambda i, cut: b_rows.at[ring(i), :, cut], bs, br, lambda *_: None)
    b = b_rows[...].reshape(RING * shard_rows, width)
    weights[1].wait()
    weights[2].wait()
    wide = act.shape[1] // 2

    @pl.loop(0, act.shape[1] // wide)
    def _(i):
        at = pl.ds(pl.multiple_of(i * wide, wide), wide)
        gate = dot(b, wg[:, at])
        act[:, at] = (gate * jax.nn.sigmoid(gate) * dot(b, wu[:, at])).astype(jnp.bfloat16)

    down_load.wait()
    inner = act[...]

    settle()
    out_ref[...] = (mid[...].astype(jnp.float32) + reduce_rows(1, lambda at: dot(inner, wd[:, at]))).astype(jnp.bfloat16)
    settle()
    for c in pending + cross:
        c.wait_send()
    for g in range(heads):
        for c in q1(g) + [q2(g, i) for i in range(6)]:
            c.wait_send()
        for c in (*first(g, 0), *first(g, 1), *second(g)):
            c().wait_send()
        swap(g).wait_send()


def layer(cache_len, hidden, gain1, gain2, cos, sin, cache_k, cache_v, w_query, w_key, w_value, w_out, w_gate, w_up, w_down):
    shard_rows, width = hidden.shape
    kv_local = w_key.shape[1] // HEAD_DIM
    heads = w_query.shape[1] // w_key.shape[1]
    rows = 2 * RING * shard_rows
    slots = cache_k.shape[0]
    total = 2 * slots + rows
    inner = w_gate.shape[1]
    deep = HEAD_DIM + 8
    assert kv_local == 2 and w_down.shape[0] >= 2 * slots and width >= 2 * RING * HEAD_DIM and inner >= (heads + 2) * HEAD_DIM and cache_k.shape[1] == 2 * RING * HEAD_DIM
    bf16, f32 = jnp.bfloat16, jnp.float32
    vmem, hbm, smem = pl.BlockSpec(memory_space=pltpu.VMEM), pl.BlockSpec(memory_space=pl.ANY), pl.BlockSpec(memory_space=pltpu.SMEM)
    dma = pltpu.SemaphoreType.DMA
    return pl.pallas_call(
        layer_kernel,
        out_shape=jax.ShapeDtypeStruct(hidden.shape, bf16),
        in_specs=[smem] + [vmem] * 5 + [hbm] * 9,
        out_specs=vmem,
        scratch_shapes=[
            pltpu.VMEM((2, RING, shard_rows, width), bf16),
            pltpu.VMEM((rows, HEAD_DIM), bf16),
            pltpu.VMEM((HEAD_DIM, rows), bf16),
            pltpu.VMEM((RING, HEAD_DIM, 2 * slots), bf16),
            pltpu.VMEM((heads, RING, RING, rows, HEAD_DIM), bf16),
            pltpu.VMEM((2 * slots, HEAD_DIM), bf16),
            pltpu.VMEM((RING, rows, rows), f32),
            pltpu.VMEM((heads, RING, RING, deep, rows), f32),
            pltpu.VMEM((heads, 2, 2, deep, rows), f32),
            pltpu.VMEM((heads, 2, RING, deep, rows), f32),
            pltpu.VMEM((heads, deep, rows), f32),
            pltpu.VMEM((heads, 2, deep, rows), f32),
            pltpu.VMEM((heads, rows, HEAD_DIM), bf16),
            pltpu.VMEM((heads, rows // 2, HEAD_DIM), bf16),
            pltpu.VMEM((2, heads, rows // 2, HEAD_DIM), bf16),
            pltpu.VMEM((total, 2 * rows), f32),
            pltpu.VMEM((total, 2 * rows), f32),
            pltpu.VMEM((1, 2 * rows), f32),
            pltpu.VMEM((1, 2 * rows), f32),
            pltpu.VMEM(w_out.shape, bf16),
            pltpu.VMEM(w_gate.shape, bf16),
            pltpu.VMEM(w_up.shape, bf16),
            pltpu.VMEM(w_down.shape, bf16),
            pltpu.VMEM((RING, shard_rows, width), f32),
            pltpu.VMEM((2, shard_rows, width), f32),
            pltpu.VMEM((2, 2, shard_rows, width), f32),
            pltpu.VMEM((shard_rows, width), bf16),
            pltpu.VMEM((RING, shard_rows, width), bf16),
            pltpu.VMEM((RING * shard_rows, inner), bf16),
            dma((3,)),
            dma((2 * RING,)),
            *(dma(shape) for shape in ((2 * RING,), (6,), (7,), (6,), (heads, 9), (heads, 2, 6), (heads, 3), (heads,)) for _ in range(2)),
            dma((4,)),
            dma((2, 10)),
            dma((2, 10)),
        ],
        compiler_params=pltpu.CompilerParams(collective_id=0, has_side_effects=True, vmem_limit_bytes=VMEM_LIMIT),
        name='attend',
    )(cache_len, hidden, gain1, gain2, cos, sin, cache_k, cache_v, w_query, w_key, w_value, w_out, w_gate, w_up, w_down)


def solution(mesh):
    devices = mesh.shape['tp'] * mesh.shape['cp']
    assert mesh.shape['tp'] == RING and mesh.shape['cp'] == 2 * RING
    token_spec = P(('dp', 'cp', 'tp'), None)
    column_spec = P(None, 'tp')
    row_spec = P('tp', None)

    def tables(cache_len, shard_rows):
        half_rows, half_dim = shard_rows // 2, HEAD_DIM // 2
        row = jnp.arange(2 * RING * shard_rows, dtype=jnp.int32)
        owner = (lax.axis_index('cp') // 2) * (2 * RING) + row // shard_rows
        r = row % shard_rows
        run = jnp.where(r < half_rows, owner, 2 * devices - 1 - owner)
        pos = cache_len[0] + run * half_rows + r % half_rows
        inv_freq = 1.0 / (ROPE_BASE ** (jnp.arange(half_dim, dtype=jnp.float32) * (2.0 / HEAD_DIM)))
        angles = pos.astype(jnp.float32)[:, None] * inv_freq[None, :]
        cos, sin = jnp.cos(angles), jnp.sin(angles)
        return jnp.concatenate([cos, cos], axis=1), jnp.concatenate([-sin, sin], axis=1)

    def device_layer(hidden, pos, cache_len, cache_k, cache_v, norm1_gain, w_query, w_key, w_value, w_out, norm2_gain, w_gate, w_up, w_down):
        cos, sin = tables(cache_len, hidden.shape[0])
        return layer(cache_len, hidden, norm1_gain, norm2_gain, cos, sin, cache_k, cache_v, w_query, w_key, w_value, w_out, w_gate, w_up, w_down)

    return jax.shard_map(device_layer, mesh=mesh, in_specs=(token_spec, P(('dp', 'cp', 'tp')), P('dp'), token_spec, token_spec, P(), column_spec, column_spec, column_spec, row_spec, P(), column_spec, column_spec, row_spec), out_specs=token_spec, check_vma=False)
```
